64 devices in a mesh: dp: 4 (over x, y), cp: 16 (over z, core).
Axes of the slice: x: 2, y: 2, z: 8, core: 2. Of those that a mesh axis runs over, the one named last changes fastest.
The devices are a block of a 4x4x8 slice.
Arguments:
- x_in: bfloat16 [8192, 3584], P(('dp', 'cp')), parts along dimension 0
- dy_in: bfloat16 [8192, 3584], P(('dp', 'cp')), parts along dimension 0
- w_q: bfloat16 [3584, 3584], replicated
- w_k: bfloat16 [3584, 512], replicated
- w_v: bfloat16 [3584, 512], replicated
- w_o: bfloat16 [3584, 3584], replicated
Outputs:
- output 1: bfloat16 [8192, 3584], P(('dp', 'cp')), parts along dimension 0
- output 2: bfloat16 [8192, 3584], P(('dp', 'cp')), parts along dimension 0
There are 4 independent parts. The reference program is written for one: setup_inputs(seed, part) draws one part's arguments, and reference() takes and returns one part's arrays. A program takes and returns all parts, laid end to end along the dimension named above; an argument that names none is the same for every part.
All inputs are finite; a program needn't handle non-finite values.
Results may differ from the reference program's by a relative error of at most 0.0109693.
Values are sent between devices in bfloat16 or wider.
A program may use at most 768 MiB of HBM per device.

```python
import math
import jax
import jax.numpy as jnp
from jax import lax

SEQ_LEN = 2048
D_MODEL = 3584
Q_HEADS = 28
KV_HEADS = 4
HEAD_DIM = 128
QUERY_BLOCK = 128

Q_GROUP = Q_HEADS // KV_HEADS
SCORE_GAIN = (0.75 * math.log(SEQ_LEN)) ** 0.25


def setup_inputs(seed: int = 0, part: int = 0) -> dict:
    key_base = jax.random.key(seed)
    key_part = jax.random.fold_in(key_base, part)
    key_x, key_dy = jax.random.split(key_part)
    key_wq, key_wk, key_wv, key_wo = jax.random.split(jax.random.key(seed + 1), 4)
    in_scale = D_MODEL ** -0.5
    out_scale = (Q_HEADS * HEAD_DIM) ** -0.5
    x_in = jax.random.normal(key_x, (SEQ_LEN, D_MODEL), jnp.float32).astype(jnp.bfloat16)
    dy_in = jax.random.normal(key_dy, (SEQ_LEN, D_MODEL), jnp.float32).astype(jnp.bfloat16)
    w_q = (jax.random.normal(key_wq, (D_MODEL, Q_HEADS * HEAD_DIM), jnp.float32) * (in_scale * SCORE_GAIN)).astype(jnp.bfloat16)
    w_k = (jax.random.normal(key_wk, (D_MODEL, KV_HEADS * HEAD_DIM), jnp.float32) * (in_scale * SCORE_GAIN)).astype(jnp.bfloat16)
    w_v = (jax.random.normal(key_wv, (D_MODEL, KV_HEADS * HEAD_DIM), jnp.float32) * in_scale).astype(jnp.bfloat16)
    w_o = (jax.random.normal(key_wo, (Q_HEADS * HEAD_DIM, D_MODEL), jnp.float32) * out_scale).astype(jnp.bfloat16)
    return {"x_in": x_in, "dy_in": dy_in, "w_q": w_q, "w_k": w_k, "w_v": w_v, "w_o": w_o}


def project(rows_in, weight):
    return jnp.dot(rows_in, weight, preferred_element_type=jnp.float32).astype(jnp.bfloat16)


def reference(x_in, dy_in, w_q, w_k, w_v, w_o):
    score_scale = HEAD_DIM ** -0.5
    n_blocks = SEQ_LEN // QUERY_BLOCK
    q_rows = project(x_in, w_q).reshape(n_blocks, QUERY_BLOCK, KV_HEADS, Q_GROUP, HEAD_DIM)
    k_rows = project(x_in, w_k).reshape(SEQ_LEN, KV_HEADS, HEAD_DIM).astype(jnp.float32)
    v_rows = project(x_in, w_v).reshape(SEQ_LEN, KV_HEADS, HEAD_DIM).astype(jnp.float32)

    def forward_block(q_blk):
        q_f = q_blk.astype(jnp.float32)
        scores = jnp.einsum("thjd,uhd->thju", q_f, k_rows) * score_scale
        lse_blk = jax.nn.logsumexp(scores, axis=-1, keepdims=True)
        prob_bf = jnp.exp(scores - lse_blk).astype(jnp.bfloat16)
        out_blk = jnp.einsum("thju,uhd->thjd", prob_bf.astype(jnp.float32), v_rows).astype(jnp.bfloat16)
        return out_blk, lse_blk

    out_blocks, lse_blocks = lax.map(forward_block, q_rows)
    out_flat = out_blocks.reshape(SEQ_LEN, Q_HEADS * HEAD_DIM)
    y_out = project(out_flat, w_o)
    do_flat = jnp.dot(dy_in, w_o.T, preferred_element_type=jnp.float32).astype(jnp.bfloat16)
    do_blocks = do_flat.reshape(n_blocks, QUERY_BLOCK, KV_HEADS, Q_GROUP, HEAD_DIM)

    def backward_block(acc_pair, block_in):
        dk_acc, dv_acc = acc_pair
        q_blk, out_blk, do_blk, lse_blk = block_in
        q_f = q_blk.astype(jnp.float32)
        do_f = do_blk.astype(jnp.float32)
        scores = jnp.einsum("thjd,uhd->thju", q_f, k_rows) * score_scale
        prob_f = jnp.exp(scores - lse_blk).astype(jnp.bfloat16).astype(jnp.float32)
        row_delta = jnp.sum(do_f * out_blk.astype(jnp.float32), axis=-1, keepdims=True)
        dprob = jnp.einsum("thjd,uhd->thju", do_f, v_rows)
        dscore = (prob_f * (dprob - row_delta)).astype(jnp.bfloat16).astype(jnp.float32)
        dq_blk = (jnp.einsum("thju,uhd->thjd", dscore, k_rows) * score_scale).astype(jnp.bfloat16)
        dk_acc = dk_acc + jnp.einsum("thju,thjd->uhd", dscore, q_f) * score_scale
        dv_acc = dv_acc + jnp.einsum("thju,thjd->uhd", prob_f, do_f)
        return (dk_acc, dv_acc), dq_blk

    zero_acc = jnp.zeros((SEQ_LEN, KV_HEADS, HEAD_DIM), jnp.float32)
    acc_final, dq_blocks = lax.scan(backward_block, (zero_acc, zero_acc), (q_rows, out_blocks, do_blocks, lse_blocks))
    dq_flat = dq_blocks.reshape(SEQ_LEN, Q_HEADS * HEAD_DIM)
    dk_flat = acc_final[0].astype(jnp.bfloat16).reshape(SEQ_LEN, KV_HEADS * HEAD_DIM)
    dv_flat = acc_final[1].astype(jnp.bfloat16).reshape(SEQ_LEN, KV_HEADS * HEAD_DIM)
    dx_acc = (jnp.dot(dq_flat, w_q.T, preferred_element_type=jnp.float32)
              + jnp.dot(dk_flat, w_k.T, preferred_element_type=jnp.float32)
              + jnp.dot(dv_flat, w_v.T, preferred_element_type=jnp.float32))
    return y_out, dx_acc.astype(jnp.bfloat16)
```

```python
import functools
import math

import jax
import jax.numpy as jnp
from jax import lax
from jax.experimental import pallas as pl
from jax.experimental.pallas import tpu as pltpu
from jax.sharding import PartitionSpec as P

HEAD_DIM = 128
MESH = pl.DeviceIdType.MESH
BF = jnp.bfloat16
F32 = jnp.float32
UP, DOWN = 0, 1


def mm(a, b):
    return jnp.dot(a, b, preferred_element_type=F32)


def mm_nt(a, b):
    return lax.dot_general(a, b, (((1,), (1,)), ((), ())), preferred_element_type=F32)


def layer_kernel(n_dev, kv_heads, q_group,
                 x_hbm, dy_hbm, wq_hbm, wk_hbm, wv_hbm, wo_hbm, y_hbm, dx_hbm,
                 x_v, dy_v, wq_v, wo_v, kv_v, kt_v, vt_v, q_v, do_v, qt_v, dot_v, o_v, dq_v,
                 s_v, p_v, ds_v, part_v, pre_v, ring_v, yacc_v, dxacc_v, fin_v, fout_v,
                 in_sem, w_sem, slab_sem, ag_send, ag_recv, pre_send, pre_recv, rs_send, rs_recv,
                 fin_send, fin_recv, out_sem):
    n_chip = n_dev // 2
    far = n_chip // 2
    tok = x_v.shape[0]
    width = x_v.shape[1]
    hd = HEAD_DIM
    gcol = q_group * hd
    kvcol = kv_heads * hd
    n_piece = width // gcol
    scale = hd ** -0.5
    scale2 = scale * math.log2(math.e)

    me = lax.axis_index("cp")
    core = lax.rem(me, 2)
    chip = me // 2
    mate = me + 1 - 2 * core

    def chip_at(off):
        return lax.rem(chip + off + n_chip, n_chip)

    near = (2 * chip_at(1) + core, 2 * chip_at(-1) + core)

    def remote(src, dst, ssem, rsem, dev):
        return pltpu.make_async_remote_copy(src_ref=src, dst_ref=dst, send_sem=ssem, recv_sem=rsem,
                                            device_id={"cp": dev}, device_id_type=MESH)

    def small_copies(hbm, buf, base):
        out = []
        for b in range(n_piece):
            out.append(pltpu.make_async_copy(hbm.at[pl.ds(b * gcol, gcol), :],
                                             buf.at[:, pl.ds(b * kvcol, kvcol)], w_sem.at[base + b]))
        return out

    def slab_copies(h, slot):
        col = h * gcol if isinstance(h, int) else pl.multiple_of(h * gcol, 128)
        return (pltpu.make_async_copy(wq_hbm.at[:, pl.ds(col, gcol)], wq_v.at[slot], slab_sem.at[slot, 0]),
                pltpu.make_async_copy(wo_hbm.at[pl.ds(col, gcol), :], wo_v.at[slot], slab_sem.at[slot, 1]))

    def src_chip(d, hop):
        return chip_at(-hop) if d == UP else chip_at(hop)

    def ag_view(h, dev, d, hop):
        if hop < far:
            return kv_v.at[h, dev]
        return kv_v.at[h, dev, d]

    def ag_ring(h, d, hop):
        ref = ag_view(h, 2 * src_chip(d, hop) + core, d, hop)
        ssem = ag_send.at[h, d] if hop == 1 else ag_send.at[h, 3 + d * (far - 1) + hop - 2]
        return remote(ref, ref, ssem, ag_recv.at[h, d * far + hop - 1], near[d])

    def ag_ring_out(h, d, hop):
        dev = me if hop == 1 else 2 * src_chip(d, hop - 1) + core
        ref = ag_view(h, dev, d, hop)
        ssem = ag_send.at[h, d] if hop == 1 else ag_send.at[h, 3 + d * (far - 1) + hop - 2]
        return remote(ref, ref, ssem, ag_recv.at[h, d * far + hop - 1], near[d])

    def ag_mate_own(h):
        ref = kv_v.at[h, me]
        return remote(ref, ref, ag_send.at[h, 2], ag_recv.at[h, 2 * far], mate)

    def ag_mate_out(h, d, hop):
        ref = ag_view(h, 2 * src_chip(d, hop) + core, d, hop)
        idx = 2 * far + 1 + d * far + hop - 1
        return remote(ref, ref, ag_send.at[h, idx], ag_recv.at[h, idx], mate)

    def ag_mate_in(h, d, hop):
        ref = ag_view(h, 2 * src_chip(d, hop) + 1 - core, d, hop)
        idx = 2 * far + 1 + d * far + hop - 1
        return remote(ref, ref, ag_send.at[h, idx], ag_recv.at[h, idx], mate)

    def ag_start(h):
        for d in (UP, DOWN):
            ag_ring_out(h, d, 1).start()
        ag_mate_own(h).start()

    def ag_level(h, hop):
        for d in (UP, DOWN):
            ag_ring(h, d, hop).wait_recv()
            if hop < far:
                ag_ring_out(h, d, hop + 1).start()
            ag_mate_out(h, d, hop).start()

    def ag_finish(h):
        ref = kv_v.at[h, mate]
        remote(ref, ref, ag_send.at[h, 2], ag_recv.at[h, 2 * far], mate).wait_recv()
        for hop in range(1, far + 1):
            for d in (UP, DOWN):
                ag_mate_in(h, d, hop).wait_recv()

    def ag_drain(h):
        ag_mate_own(h).wait_send()
        for d in (UP, DOWN):
            for hop in range(1, far + 1):
                ag_ring_out(h, d, hop).wait_send()
                ag_mate_out(h, d, hop).wait_send()

    def pre_copy(h, c):
        slot = lax.rem(h, 2)
        return remote(part_v.at[slot, 1 - core, pl.ds(2 * c, 2)], pre_v.at[slot, pl.ds(2 * c, 2)],
                      pre_send.at[h, c], pre_recv.at[h, c], mate)

    def chain_len(ch):
        return far - ch

    def rs_index(ch, lvl):
        return lvl if ch == 0 else far + lvl

    def rs_dest(d, ch, lvl):
        dist = chain_len(ch) - lvl
        to = chip_at(dist) if d == UP else chip_at(-dist)
        half = ch if d == UP else 1 - ch
        return 2 * to + half

    def rs_copy(h, d, ch, lvl):
        slot = lax.rem(h, 2)
        i = rs_index(ch, lvl)
        src = part_v.at[slot, core, rs_dest(d, ch, 0)] if lvl == 0 else ring_v.at[h, d, rs_index(ch, lvl - 1)]
        return remote(src, ring_v.at[h, d, i], rs_send.at[h, d, i], rs_recv.at[h, d, i], near[d])

    def rs_begin(h):
        slot = lax.rem(h, 2)
        for c in range(n_chip):
            pre_copy(h, c).wait()
        for e in range(n_dev):
            part_v[slot, core, e] = part_v[slot, core, e] + pre_v[slot, e]
        for d in (UP, DOWN):
            for ch in (0, 1):
                rs_copy(h, d, ch, 0).start()

    def rs_level(h, lvl):
        slot = lax.rem(h, 2)
        for ch in (0, 1):
            if lvl < chain_len(ch):
                for d in (UP, DOWN):
                    rs_copy(h, d, ch, lvl - 1).wait_recv()
                    i = rs_index(ch, lvl - 1)
                    ring_v[h, d, i] = ring_v[h, d, i] + part_v[slot, core, rs_dest(d, ch, lvl)]
                    rs_copy(h, d, ch, lvl).start()

    def fin_copy(h):
        return remote(fout_v.at[h], fin_v.at[core, h], fin_send.at[h], fin_recv.at[h], mate)

    def rs_end(h):
        slot = lax.rem(h, 2)
        for ch in (0, 1):
            for d in (UP, DOWN):
                rs_copy(h, d, ch, chain_len(ch) - 1).wait_recv()
        factor = jnp.where(core == 0, scale, 1.0).astype(F32)
        for half in (0, 1):
            up = ring_v[h, UP, rs_index(half, chain_len(half) - 1)]
            dn = ring_v[h, DOWN, rs_index(1 - half, chain_len(1 - half) - 1)]
            total = (part_v[slot, core, 2 * chip + half] + up + dn) * factor
            done = total.astype(BF)

            @pl.when(core == half)
            def _():
                fin_v[core, h] = done

            @pl.when(core != half)
            def _():
                fout_v[h] = done
        fin_copy(h).start()
        for ch in (0, 1):
            for lvl in range(chain_len(ch)):
                for d in (UP, DOWN):
                    rs_copy(h, d, ch, lvl).wait_send()

    def project_q(slot):
        q = mm(x_v[...], wq_v[slot]).astype(BF)
        q_v[slot] = q

    def project_do(slot):
        do_v[slot] = mm_nt(dy_v[...], wo_v[slot]).astype(BF)

    def transpose_kv(h):
        for e in range(n_dev):
            kt_v[:, e * tok:(e + 1) * tok] = kv_v[h, e, 0].T
            vt_v[:, e * tok:(e + 1) * tok] = kv_v[h, e, 1].T

    n_key = n_dev * tok
    chunk = 2 * tok

    def stage_scores(slot, j):
        cols = slice(j * hd, (j + 1) * hd)
        q_j = q_v[slot, :, cols]
        qt_v[:, cols] = q_j.T
        dot_v[:, cols] = do_v[slot, :, cols].T
        part_max = None
        for n in range(n_key // chunk):
            s = mm(q_j, kt_v[:, n * chunk:(n + 1) * chunk]) * scale2
            s_v[:, n * chunk:(n + 1) * chunk] = s
            for i in range(chunk // 128):
                piece = s[:, i * 128:(i + 1) * 128]
                part_max = piece if part_max is None else jnp.maximum(part_max, piece)
        row_max = jnp.max(part_max, axis=1, keepdims=True)
        for r in range(0, tok, 16):
            e = jnp.exp2(s_v[r:r + 16, :] - row_max[r:r + 16])
            total = jnp.sum(e, axis=1, keepdims=True)
            p_v[j * tok + r:j * tok + r + 16, :] = (e * (1.0 / total)).astype(BF)

    def stage_grads(h, slot, j):
        cols = slice(j * hd, (j + 1) * hd)
        rows = slice(j * tok, (j + 1) * tok)
        v_all = kv_v[h, :, 1].reshape(n_key, hd)
        out = mm(p_v[rows, :], v_all).astype(BF)
        o_v[slot, :, cols] = out
        do_j = do_v[slot, :, cols]
        delta = jnp.sum(out.astype(F32) * do_j.astype(F32), axis=1, keepdims=True)
        for n in range(n_key // chunk):
            kc = slice(n * chunk, (n + 1) * chunk)
            dp = mm(do_j, vt_v[:, kc])
            ds_v[rows, kc] = (p_v[rows, kc].astype(F32) * (dp - delta)).astype(BF)
        k_all = kv_v[h, :, 0].reshape(n_key, hd)
        dq_v[slot, :, cols] = (mm(ds_v[rows, :], k_all) * scale).astype(BF)

    def key_grads(h):
        slot = lax.rem(h, 2)
        for c in range(n_chip):
            kc = slice(c * chunk, (c + 1) * chunk)
            gk = mm(qt_v[...], ds_v[:, kc])
            gv = mm(dot_v[...], p_v[:, kc])
            for half in (0, 1):
                part_v[slot, 0, 2 * c + half] = gk[:, half * tok:(half + 1) * tok]
                part_v[slot, 1, 2 * c + half] = gv[:, half * tok:(half + 1) * tok]
            pre_copy(h, c).start()

    def outputs_y(slot):
        for b in range(n_piece):
            cols = slice(b * gcol, (b + 1) * gcol)
            yacc_v[:, cols] += mm(o_v[slot], wo_v[slot, :, cols])

    def outputs_dx(slot):
        for b in range(n_piece):
            cols = slice(b * gcol, (b + 1) * gcol)
            dxacc_v[:, cols] += mm_nt(dq_v[slot], wq_v[slot, cols, :])

    x_copy = pltpu.make_async_copy(x_hbm, x_v, in_sem.at[0])
    dy_copy = pltpu.make_async_copy(dy_hbm, dy_v, in_sem.at[1])
    x_copy.start()
    wk_in = small_copies(wk_hbm, p_v, 0)
    wv_in = small_copies(wv_hbm, ds_v, n_piece)
    for copy in wk_in + wv_in:
        copy.start()

    barrier = pltpu.get_barrier_semaphore()
    for dev in (near[UP], near[DOWN], mate):
        pl.semaphore_signal(barrier, inc=1, device_id={"cp": dev}, device_id_type=MESH)

    yacc_v[...] = jnp.zeros_like(yacc_v)
    dxacc_v[...] = jnp.zeros_like(dxacc_v)
    x_copy.wait()

    def project_small(copies, buf, which):
        acc = None
        for b in range(n_piece):
            copies[b].wait()
            term = mm(x_v[:, b * gcol:(b + 1) * gcol], buf[:, b * kvcol:(b + 1) * kvcol])
            acc = term if acc is None else acc + term
        acc = acc.astype(BF)
        for h in range(kv_heads):
            kv_v[h, me, which] = acc[:, h * hd:(h + 1) * hd]

    project_small(wk_in, p_v, 0)
    for copy in slab_copies(0, 0):
        copy.start()
    dy_copy.start()
    project_small(wv_in, ds_v, 1)
    pl.semaphore_wait(barrier, 3)
    for h in (0, 1):
        ag_start(h)
    for copy in slab_copies(1, 1):
        copy.start()
    dy_copy.wait()
    slab_copies(0, 0)[0].wait()
    project_q(0)
    for h in (0, 1):
        ag_level(h, 1)
    slab_copies(0, 0)[1].wait()
    project_do(0)
    for h in (0, 1):
        ag_level(h, 2)
    slab_copies(1, 1)[0].wait()
    project_q(1)
    for h in (0, 1):
        ag_level(h, 3)
    for h in range(2, kv_heads):
        ag_start(h)
    slab_copies(1, 1)[1].wait()
    project_do(1)
    for h in (0, 1):
        ag_level(h, 4)

    def head_step(h, carry):
        slot = lax.rem(h, 2)
        ag_finish(h)
        transpose_kv(h)
        stage_scores(slot, 0)
        for j in range(q_group):
            if j in (0, 2, 4, 6):
                @pl.when(h == 0)
                def _():
                    for g in range(2, kv_heads):
                        ag_level(g, j // 2 + 1)
            if j in (0, 3, 6):
                @pl.when(h >= 1)
                def _():
                    rs_level(h - 1, j // 3 + 1)
            if j == 1:
                @pl.when(h >= 2)
                def _():
                    rs_end(h - 2)
            if j + 1 < q_group:
                stage_scores(slot, j + 1)
            stage_grads(h, slot, j)
        key_grads(h)

        @pl.when(h + 2 < kv_heads)
        def _():
            outputs_y(slot)
            outputs_dx(slot)
            for copy in slab_copies(h + 2, slot):
                copy.start()

        rs_begin(h)

        @pl.when((h >= 1) & (h + 1 < kv_heads))
        def _():
            for copy in slab_copies(h + 1, 1 - slot):
                copy.wait()
            project_q(1 - slot)
            project_do(1 - slot)

        return carry

    lax.fori_loop(0, kv_heads, head_step, 0)

    last = kv_heads - 1
    wk_in = small_copies(wk_hbm, p_v, 0)
    wv_in = small_copies(wv_hbm, ds_v, n_piece)
    for copy in wk_in + wv_in:
        copy.start()
    slot_a, slot_b = (last - 1) % 2, last % 2
    outputs_y(slot_a)
    rs_level(last, 1)
    rs_end(last - 1)
    outputs_dx(slot_a)
    rs_level(last, 2)
    outputs_y(slot_b)
    rs_level(last, 3)
    x_v[...] = yacc_v[...].astype(BF)
    y_copy = pltpu.make_async_copy(x_v, y_hbm, out_sem.at[0])
    y_copy.start()
    outputs_dx(slot_b)
    rs_end(last)
    for h in range(kv_heads):
        remote(fout_v.at[h], fin_v.at[1 - core, h], fin_send.at[h], fin_recv.at[h], mate).wait_recv()
    for copy in wk_in + wv_in:
        copy.wait()
    gk = jnp.concatenate([fin_v[0, h].T for h in range(kv_heads)], axis=1)
    gv = jnp.concatenate([fin_v[1, h].T for h in range(kv_heads)], axis=1)
    for b in range(n_piece):
        cols = slice(b * gcol, (b + 1) * gcol)
        kcols = slice(b * kvcol, (b + 1) * kvcol)
        total = dxacc_v[:, cols] + mm_nt(gk, p_v[:, kcols]) + mm_nt(gv, ds_v[:, kcols])
        dy_v[:, cols] = total.astype(BF)
    dx_copy = pltpu.make_async_copy(dy_v, dx_hbm, out_sem.at[1])
    dx_copy.start()
    for h in range(kv_heads):
        ag_drain(h)
        fin_copy(h).wait_send()
    y_copy.wait()
    dx_copy.wait()


def solution(mesh):
    n_dev = mesh.shape["cp"]
    row_spec = P(("dp", "cp"), None)
    full_spec = P(None, None)

    def local_body(x_loc, dy_loc, w_q, w_k, w_v, w_o):
        tok, width = x_loc.shape
        q_heads = w_q.shape[1] // HEAD_DIM
        kv_heads = w_k.shape[1] // HEAD_DIM
        q_group = q_heads // kv_heads
        gcol = q_group * HEAD_DIM
        n_key = tok * n_dev
        far = n_dev // 4
        hd = HEAD_DIM
        any_spec = pl.BlockSpec(memory_space=pl.ANY)
        dma = pltpu.SemaphoreType.DMA
        scratch = [
            pltpu.VMEM((tok, width), BF), pltpu.VMEM((tok, width), BF),
            pltpu.VMEM((2, width, gcol), BF), pltpu.VMEM((2, gcol, width), BF),
            pltpu.VMEM((kv_heads, n_dev, 2, tok, hd), BF),
            pltpu.VMEM((hd, n_key), BF), pltpu.VMEM((hd, n_key), BF),
            pltpu.VMEM((2, tok, gcol), BF), pltpu.VMEM((2, tok, gcol), BF),
            pltpu.VMEM((hd, q_group * tok), BF), pltpu.VMEM((hd, q_group * tok), BF),
            pltpu.VMEM((2, tok, gcol), BF), pltpu.VMEM((2, tok, gcol), BF),
            pltpu.VMEM((tok, n_key), F32),
            pltpu.VMEM((q_group * tok, n_key), BF), pltpu.VMEM((q_group * tok, n_key), BF),
            pltpu.VMEM((2, 2, n_dev, hd, tok), F32), pltpu.VMEM((2, n_dev, hd, tok), F32),
            pltpu.VMEM((kv_heads, 2, 2 * far - 1, hd, tok), F32),
            pltpu.VMEM((tok, width), F32), pltpu.VMEM((tok, width), F32),
            pltpu.VMEM((2, kv_heads, hd, tok), BF), pltpu.VMEM((kv_heads, hd, tok), BF),
            dma((2,)), dma((2 * (width // gcol),)), dma((2, 2)),
            dma((kv_heads, 4 * far + 1)), dma((kv_heads, 4 * far + 1)),
            dma((kv_heads, n_dev // 2)), dma((kv_heads, n_dev // 2)),
            dma((kv_heads, 2, 2 * far - 1)), dma((kv_heads, 2, 2 * far - 1)),
            dma((kv_heads,)), dma((kv_heads,)), dma((2,)),
        ]
        out = jax.ShapeDtypeStruct((tok, width), BF)
        return pl.pallas_call(
            functools.partial(layer_kernel, n_dev, kv_heads, q_group),
            out_shape=(out, out),
            in_specs=[any_spec] * 6,
            out_specs=(any_spec, any_spec),
            scratch_shapes=scratch,
            name="layer",
            compiler_params=pltpu.CompilerParams(collective_id=0, has_side_effects=True,
                                                 vmem_limit_bytes=67043328),
        )(x_loc, dy_loc, w_q, w_k, w_v, w_o)

    return jax.shard_map(local_body, mesh=mesh,
                         in_specs=(row_spec, row_spec, full_spec, full_spec, full_spec, full_spec),
                         out_specs=(row_spec, row_spec), check_vma=False)
```

```python
import functools
import math

import jax
import jax.numpy as jnp
from jax import lax
from jax.experimental import pallas as pl
from jax.experimental.pallas import tpu as pltpu
from jax.sharding import PartitionSpec as P

HEAD_DIM = 128
MESH = pl.DeviceIdType.MESH
BF = jnp.bfloat16
F32 = jnp.float32
UP, DOWN = 0, 1


def mm(a, b):
    return jnp.dot(a, b, preferred_element_type=F32)


def mm_nt(a, b):
    return lax.dot_general(a, b, (((1,), (1,)), ((), ())), preferred_element_type=F32)


def layer_kernel(n_dev, kv_heads, q_group,
                 x_hbm, dy_hbm, wq_hbm, wk_hbm, wv_hbm, wo_hbm, y_hbm, dx_hbm,
                 x_v, dy_v, wq_v, wo_v, kv_v, kt_v, vt_v, q_v, do_v, qt_v, dot_v,
                 s_v, p_v, ds_v, part_v, pre_v, ring_v, yacc_v, dxacc_v, fin_v, fout_v,
                 in_sem, w_sem, slab_sem, ag_send, ag_recv, pre_send, pre_recv, rs_send, rs_recv,
                 fin_send, fin_recv, out_sem):
    n_chip = n_dev // 2
    far = n_chip // 2
    tok = x_v.shape[0]
    width = x_v.shape[1]
    hd = HEAD_DIM
    gcol = q_group * hd
    kvcol = kv_heads * hd
    n_piece = width // gcol
    n_key = n_dev * tok
    chunk = 2 * tok
    scale = hd ** -0.5
    scale2 = scale * math.log2(math.e)

    me = lax.axis_index("cp")
    core = lax.rem(me, 2)
    chip = me // 2
    mate = me + 1 - 2 * core

    def chip_at(off):
        return lax.rem(chip + off + n_chip, n_chip)

    near = (2 * chip_at(1) + core, 2 * chip_at(-1) + core)

    def remote(src, dst, ssem, rsem, dev):
        return pltpu.make_async_remote_copy(src_ref=src, dst_ref=dst, send_sem=ssem, recv_sem=rsem,
                                            device_id={"cp": dev}, device_id_type=MESH)

    def small_copies(hbm, buf, base):
        return [pltpu.make_async_copy(hbm.at[pl.ds((i // 2) * gcol, gcol), pl.ds((i % 2) * chunk, chunk)],
                                      buf.at[i], w_sem.at[base + i]) for i in range(n_chip)]

    def col_of(h):
        return h * gcol if isinstance(h, int) else pl.multiple_of(h * gcol, 128)

    def slab_q(h, slot):
        return pltpu.make_async_copy(wq_hbm.at[:, pl.ds(col_of(h), gcol)], wq_v.at[slot], slab_sem.at[slot, 0])

    def slab_o(h, slot):
        return pltpu.make_async_copy(wo_hbm.at[pl.ds(col_of(h), gcol), :], wo_v.at[slot], slab_sem.at[slot, 1])

    def src_chip(d, hop):
        return chip_at(-hop) if d == UP else chip_at(hop)

    def ag_view(h, dev, d, hop):
        if hop < far:
            return kv_v.at[h, dev]
        return kv_v.at[h, dev, d]

    def ag_ring(h, d, hop):
        ref = ag_view(h, 2 * src_chip(d, hop) + core, d, hop)
        return remote(ref, ref, ag_send.at[h], ag_recv.at[h, d * far + hop - 1], near[d])

    def ag_ring_out(h, d, hop):
        dev = me if hop == 1 else 2 * src_chip(d, hop - 1) + core
        ref = ag_view(h, dev, d, hop)
        return remote(ref, ref, ag_send.at[h], ag_recv.at[h, d * far + hop - 1], near[d])

    def ag_mate_own(h):
        ref = kv_v.at[h, me]
        return remote(ref, ref, ag_send.at[h], ag_recv.at[h, 2 * far], mate)

    def ag_mate_out(h, d, hop):
        ref = ag_view(h, 2 * src_chip(d, hop) + core, d, hop)
        idx = 2 * far + 1 + d * far + hop - 1
        return remote(ref, ref, ag_send.at[h], ag_recv.at[h, idx], mate)

    def ag_mate_in(h, d, hop):
        ref = ag_view(h, 2 * src_chip(d, hop) + 1 - core, d, hop)
        idx = 2 * far + 1 + d * far + hop - 1
        return remote(ref, ref, ag_send.at[h], ag_recv.at[h, idx], mate)

    def ag_start(h):
        for d in (UP, DOWN):
            ag_ring_out(h, d, 1).start()
        ag_mate_own(h).start()

    def ag_level(h, hop):
        for d in (UP, DOWN):
            ag_ring(h, d, hop).wait_recv()
            if hop < far:
                ag_ring_out(h, d, hop + 1).start()
            ag_mate_out(h, d, hop).start()

    def ag_finish(h):
        ref = kv_v.at[h, mate]
        remote(ref, ref, ag_send.at[h], ag_recv.at[h, 2 * far], mate).wait_recv()
        for hop in range(1, far + 1):
            for d in (UP, DOWN):
                ag_mate_in(h, d, hop).wait_recv()

    def ag_drain(h):
        ref = kv_v.at[h, pl.ds(0, n_dev - 1)]
        remote(ref, ref, ag_send.at[h], ag_recv.at[h, 0], mate).wait_send()

    def slot_of(off):
        return off % n_chip

    def pre_copy(h, off):
        slot, i = lax.rem(h, 2), slot_of(off)
        return remote(part_v.at[slot, 1 - core, i], pre_v.at[h, i], pre_send.at[h], pre_recv.at[h, i], mate)

    def chain_len(ch):
        return far - ch

    def rs_index(ch, lvl):
        return lvl if ch == 0 else far + lvl

    def rs_place(d, ch, lvl):
        dist = chain_len(ch) - lvl
        return slot_of(dist if d == UP else -dist), (ch if d == UP else 1 - ch)

    def rs_copy(h, d, ch, lvl):
        i = rs_index(ch, lvl)
        if lvl == 0:
            off, half = rs_place(d, ch, 0)
            src = part_v.at[lax.rem(h, 2), core, off, half]
        else:
            src = ring_v.at[h, d, rs_index(ch, lvl - 1)]
        return remote(src, ring_v.at[h, d, i], rs_send.at[h], rs_recv.at[h, d, i], near[d])

    def rs_begin(h):
        slot = lax.rem(h, 2)
        for off in (far, far - 1, 1 - far):
            pre_copy(h, off).wait_recv()
        for ch in (0, 1):
            for d in (UP, DOWN):
                off, half = rs_place(d, ch, 0)
                part_v[slot, core, off, half] = part_v[slot, core, off, half] + pre_v[h, off, half]
                rs_copy(h, d, ch, 0).start()

    def rs_step(h, ch, lvl):
        slot = lax.rem(h, 2)
        places = [rs_place(d, ch, lvl) for d in (UP, DOWN)]
        if ch == 1:
            for off, _ in places:
                pre_copy(h, off).wait_recv()
        mine = [part_v[slot, core, off, half] + pre_v[h, off, half] for off, half in places]
        i = rs_index(ch, lvl - 1)
        for d in (UP, DOWN):
            rs_copy(h, d, ch, lvl - 1).wait_recv()
            ring_v[h, d, i] = ring_v[h, d, i] + mine[d]
            rs_copy(h, d, ch, lvl).start()

    def fin_copy(h):
        return remote(fout_v.at[h], fin_v.at[core, h], fin_send.at[h], fin_recv.at[h], mate)

    def rs_end(h):
        slot = lax.rem(h, 2)
        pre_copy(h, 0).wait_recv()
        for ch in (0, 1):
            for d in (UP, DOWN):
                rs_copy(h, d, ch, chain_len(ch) - 1).wait_recv()
        factor = jnp.where(core == 0, scale, 1.0).astype(F32)
        for half in (0, 1):
            up = ring_v[h, UP, rs_index(half, chain_len(half) - 1)]
            dn = ring_v[h, DOWN, rs_index(1 - half, chain_len(1 - half) - 1)]
            total = (part_v[slot, core, 0, half] + pre_v[h, 0, half] + up + dn) * factor
            done = total.astype(BF)

            @pl.when(core == half)
            def _():
                fin_v[core, h] = done

            @pl.when(core != half)
            def _():
                fout_v[h] = done
        fin_copy(h).start()
        remote(ring_v.at[h], ring_v.at[h], rs_send.at[h], rs_recv.at[h, 0, 0], near[UP]).wait_send()
        remote(pre_v.at[h], pre_v.at[h], pre_send.at[h], pre_recv.at[h, 0], mate).wait_send()

    def project_q(h, slot):
        q_v[h] = mm(x_v[...], wq_v[slot]).astype(BF)

    do_cut = (gcol // 2 + chunk - 1) // chunk * chunk

    def project_do(h, slot, part):
        cols = slice(0, do_cut) if part == 0 else slice(do_cut, gcol)
        do_v[h, :, cols] = mm_nt(dy_v[...], wo_v[slot, cols, :]).astype(BF)

    def transpose_kv(h):
        for e in range(n_dev):
            c, cols = e // 2, slice((e % 2) * tok, (e % 2 + 1) * tok)
            kt_v[c, :, cols] = kv_v[h, e, 0].T
            vt_v[c, :, cols] = kv_v[h, e, 1].T

    blk = 16
    n_blk = tok // blk

    def attend(h, serve):
        row_max, delta = {}, {}

        def lanes(j):
            return slice(j * hd, (j + 1) * hd)

        def rows(j):
            return slice(j * tok, (j + 1) * tok)

        def scores(j, i, state):
            if i == 0:
                qt_v[:, lanes(j)] = q_v[h, :, lanes(j)].T
                dot_v[:, lanes(j)] = do_v[h, :, lanes(j)].T
            s = mm(q_v[h, :, lanes(j)], kt_v[i]) * scale2
            s_v[j % 2, i] = s
            top = jnp.maximum(s[:, :hd], s[:, hd:])
            state["top"] = top if i == 0 else jnp.maximum(state["top"], top)
            if i == n_chip - 1:
                row_max[j] = jnp.max(state["top"], axis=1, keepdims=True)

        def exps(j, i, state):
            r = slice(i * blk, (i + 1) * blk)
            total = None
            for c in range(n_chip):
                e = jnp.exp2(s_v[j % 2, c, r, :] - row_max[j][r])
                s_v[j % 2, c, r, :] = e
                both = e[:, :hd] + e[:, hd:]
                total = both if total is None else total + both
            state[i] = 1.0 / jnp.sum(total, axis=1, keepdims=True)

        def probs(j, i, state):
            r = slice(i * blk, (i + 1) * blk)
            for c in range(n_chip):
                p_v[c, j * tok + i * blk:j * tok + (i + 1) * blk, :] = (s_v[j % 2, c, r, :] * state[i]).astype(BF)

        def kv_chunk(i, which):
            return kv_v[h, 2 * i:2 * i + 2, which].reshape(chunk, hd)

        def add_to(state, name, term):
            state[name] = term if name not in state else state[name] + term

        for b in range(-2, q_group + 1):
            state = {}
            soft = {}
            serve(b)
            for i in range(n_chip + 1):
                if i < n_chip and 0 <= b - 1 < q_group:
                    add_to(state, "dq", mm(ds_v[i, rows(b - 1), :], kv_chunk(i, 0)))
                if i < n_chip and 0 <= b + 2 < q_group:
                    scores(b + 2, i, state)
                if 0 <= b + 1 < q_group:
                    if i < n_blk:
                        exps(b + 1, i, soft)
                    if i > 0:
                        probs(b + 1, i - 1, soft)
            if 0 <= b - 1 < q_group:
                do_v[h, :, lanes(b - 1)] = (state["dq"] * scale).astype(BF)
            for i in range(n_chip):
                if 0 <= b + 1 < q_group:
                    add_to(state, "out", mm(p_v[i, rows(b + 1), :], kv_chunk(i, 1)))
                if 0 <= b < q_group:
                    dp = mm(do_v[h, :, lanes(b)], vt_v[i])
                    ds_v[i, rows(b), :] = (p_v[i, rows(b), :].astype(F32) * (dp - delta[b])).astype(BF)
            if 0 <= b + 1 < q_group:
                out = state["out"].astype(BF)
                q_v[h, :, lanes(b + 1)] = out
                do_j = do_v[h, :, lanes(b + 1)].astype(F32)
                delta[b + 1] = jnp.sum(out.astype(F32) * do_j, axis=1, keepdims=True)

    def key_grads(h):
        slot = lax.rem(h, 2)
        order = [far]
        for dist in range(far - 1, 0, -1):
            order += [dist, -dist]
        order.append(0)
        for group in (order[:3], order[3:]):
            for off in group:
                c = chip_at(off)
                gk = mm(qt_v[...], ds_v[c])
                gv = mm(dot_v[...], p_v[c])
                for half in (0, 1):
                    part_v[slot, 0, slot_of(off), half] = gk[:, half * tok:(half + 1) * tok]
                    part_v[slot, 1, slot_of(off), half] = gv[:, half * tok:(half + 1) * tok]
            for off in group:
                pre_copy(h, off).start()

    def outputs_y(h, slot):
        for b in range(n_piece):
            cols = slice(b * gcol, (b + 1) * gcol)
            yacc_v[:, cols] += mm(q_v[h], wo_v[slot, :, cols])

    def outputs_dx(h, slot):
        for b in range(n_piece):
            cols = slice(b * gcol, (b + 1) * gcol)
            dxacc_v[:, cols] += mm_nt(do_v[h], wq_v[slot, cols, :])

    x_copy = pltpu.make_async_copy(x_hbm, x_v, in_sem.at[0])
    dy_copy = pltpu.make_async_copy(dy_hbm, dy_v, in_sem.at[1])
    x_copy.start()
    wk_in = small_copies(wk_hbm, p_v, 0)
    wv_in = small_copies(wv_hbm, ds_v, n_chip)
    for copy in wk_in:
        copy.start()

    barrier = pltpu.get_barrier_semaphore()
    for dev in (near[UP], near[DOWN], mate):
        pl.semaphore_signal(barrier, inc=1, device_id={"cp": dev}, device_id_type=MESH)

    yacc_v[...] = jnp.zeros_like(yacc_v)
    dxacc_v[...] = jnp.zeros_like(dxacc_v)
    for copy in wv_in:
        copy.start()
    x_copy.wait()

    def project_small(buf, which):
        acc = [None, None]
        for i in range(n_chip):
            b, half = i // 2, i % 2
            term = mm(x_v[:, b * gcol:(b + 1) * gcol], buf[i])
            acc[half] = term if b == 0 else acc[half] + term
        for h in range(kv_heads):
            col = (h % 2) * hd
            kv_v[h, me, which] = acc[h // 2][:, col:col + hd].astype(BF)

    for copy in wk_in:
        copy.wait()
    slab_q(2, 0).start()
    project_small(p_v, 0)
    for copy in wv_in:
        copy.wait()
    dy_copy.start()
    project_small(ds_v, 1)
    slab_o(2, 0).start()
    pl.semaphore_wait(barrier, 3)
    ag_start(0)
    ag_start(1)

    slab_q(2, 0).wait()
    slab_q(1, 1).start()
    project_q(2, 0)
    slab_o(1, 1).start()
    dy_copy.wait()
    slab_o(2, 0).wait()
    slab_q(0, 0).start()
    project_do(2, 0, 0)
    ag_level(0, 1)
    project_do(2, 0, 1)
    slab_o(0, 0).start()
    ag_level(1, 1)
    slab_q(1, 1).wait()
    project_q(1, 1)
    ag_level(0, 2)
    slab_o(1, 1).wait()
    project_do(1, 1, 0)
    ag_level(1, 2)
    ag_start(2)
    project_do(1, 1, 1)
    ag_level(0, 3)
    slab_q(0, 0).wait()
    project_q(0, 0)
    ag_level(1, 3)
    slab_o(0, 0).wait()
    project_do(0, 0, 0)
    ag_level(0, 4)
    ag_level(2, 1)
    ag_start(3)
    project_do(0, 0, 1)
    ag_level(1, 4)

    first_serve = {-2: [(2, 2)], 1: [(3, 1)], 2: [(2, 3)], 4: [(3, 2)], 5: [(2, 4)], 7: [(3, 3)]}

    def head_step(h, carry):
        def serve(b):
            if b in first_serve:
                @pl.when(h == 0)
                def _():
                    for g, hop in first_serve[b]:
                        ag_level(g, hop)
            if b in (-2, 1, 4, 6):
                @pl.when((h == 1) | (h == 3))
                def _():
                    if b == -2:
                        @pl.when(h == 3)
                        def _():
                            rs_step(h - 2, 0, 3)
                        rs_step(h - 1, 0, 1)
                    elif b == 1:
                        rs_step(h - 1, 1, 1)
                    elif b == 4:
                        rs_step(h - 1, 0, 2)

                        @pl.when(h == 3)
                        def _():
                            rs_end(h - 2)
                    else:
                        rs_step(h - 1, 1, 2)
            if b in (3, 5):
                @pl.when(h == 2)
                def _():
                    if b == 3:
                        rs_end(h - 2)
                        rs_step(h - 1, 0, 1)
                    else:
                        rs_step(h - 1, 1, 1)

        ag_finish(h)
        transpose_kv(h)
        attend(h, serve)
        key_grads(h)

        @pl.when(h == 2)
        def _():
            rs_step(h - 1, 0, 2)

        rs_begin(h)

        @pl.when(h == 0)
        def _():
            outputs_y(h, 0)
            slab_o(3, 0).start()
            ag_level(3, 4)
            outputs_dx(h, 0)
            slab_q(3, 0).start()

        @pl.when(h == 1)
        def _():
            rs_step(h - 1, 0, 3)

        @pl.when(h == 2)
        def _():
            slab_q(3, 0).wait()
            project_q(3, 0)
            rs_step(h - 1, 1, 2)
            slab_o(3, 0).wait()
            project_do(3, 0, 0)
            project_do(3, 0, 1)

        return carry

    lax.fori_loop(0, kv_heads, head_step, 0)

    last = kv_heads - 1
    wk_in = small_copies(wk_hbm, p_v, 0)
    wv_in = small_copies(wv_hbm, ds_v, n_chip)
    for copy in wk_in + wv_in:
        copy.start()

    def fin_wait(h):
        remote(fout_v.at[h], fin_v.at[1 - core, h], fin_send.at[h], fin_recv.at[h], mate).wait_recv()

    def dx_copy(b):
        cols = pl.ds(b * gcol, gcol)
        return pltpu.make_async_copy(dy_v.at[:, cols], dx_hbm.at[:, cols], out_sem.at[b])

    def key_outputs(half, store):
        pair = (2 * half, 2 * half + 1)
        gk = jnp.concatenate([fin_v[0, h].T for h in pair], axis=1)
        gv = jnp.concatenate([fin_v[1, h].T for h in pair], axis=1)
        for b in range(n_piece):
            cols = slice(b * gcol, (b + 1) * gcol)
            i = 2 * b + half
            total = dxacc_v[:, cols] + mm_nt(gk, p_v[i]) + mm_nt(gv, ds_v[i])
            if store:
                dy_v[:, cols] = total.astype(BF)
                dx_copy(b).start()
            else:
                dxacc_v[:, cols] = total

    rs_step(2, 0, 3)
    outputs_y(1, 1)
    slab_o(2, 1).start()
    outputs_dx(1, 1)
    slab_q(2, 1).start()
    rs_step(3, 0, 1)
    outputs_y(3, 0)
    rs_step(3, 1, 1)
    outputs_dx(3, 0)
    rs_end(2)
    rs_step(3, 0, 2)
    slab_o(2, 1).wait()
    outputs_y(2, 1)
    x_v[...] = yacc_v[...].astype(BF)
    y_copy = pltpu.make_async_copy(x_v, y_hbm, in_sem.at[0])
    y_copy.start()
    rs_step(3, 1, 2)
    for copy in wk_in + wv_in:
        copy.wait()
    fin_wait(0)
    fin_wait(1)
    key_outputs(0, False)
    rs_step(3, 0, 3)
    slab_q(2, 1).wait()
    outputs_dx(2, 1)
    for h in range(kv_heads):
        ag_drain(h)
    rs_end(3)
    fin_wait(2)
    fin_wait(3)
    key_outputs(1, True)
    for h in range(kv_heads):
        fin_copy(h).wait_send()
    y_copy.wait()
    for b in range(n_piece):
        dx_copy(b).wait()


def store_kernel(y_in, dx_in, y_out, dx_out, buf, in_sem, out_sem):
    n_part, rows = buf.shape[0] // 2, buf.shape[1]
    pairs = []
    for i in range(2 * n_part):
        src, dst = ((y_in, y_out), (dx_in, dx_out))[i // n_part]
        at = pl.ds((i % n_part) * rows, rows)
        pairs.append((pltpu.make_async_copy(src.at[at], buf.at[i], in_sem.at[i]),
                      pltpu.make_async_copy(buf.at[i], dst.at[at], out_sem.at[i])))
    for take, _ in pairs:
        take.start()
    for take, give in pairs:
        take.wait()
        give.start()
    for _, give in pairs:
        give.wait()


def solution(mesh):
    n_dev = mesh.shape["cp"]
    row_spec = P(("dp", "cp"), None)
    full_spec = P(None, None)

    def local_body(x_loc, dy_loc, w_q, w_k, w_v, w_o):
        tok, width = x_loc.shape
        q_heads = w_q.shape[1] // HEAD_DIM
        kv_heads = w_k.shape[1] // HEAD_DIM
        q_group = q_heads // kv_heads
        gcol = q_group * HEAD_DIM
        n_chip = n_dev // 2
        far = n_chip // 2
        chunk = 2 * tok
        hd = HEAD_DIM
        any_spec = pl.BlockSpec(memory_space=pl.ANY)
        dma = pltpu.SemaphoreType.DMA
        scratch = [
            pltpu.VMEM((tok, width), BF), pltpu.VMEM((tok, width), BF),
            pltpu.VMEM((2, width, gcol), BF), pltpu.VMEM((2, gcol, width), BF),
            pltpu.VMEM((kv_heads, n_dev, 2, tok, hd), BF),
            pltpu.VMEM((n_chip, hd, chunk), BF), pltpu.VMEM((n_chip, hd, chunk), BF),
            pltpu.VMEM((kv_heads, tok, gcol), BF), pltpu.VMEM((kv_heads, tok, gcol), BF),
            pltpu.VMEM((hd, q_group * tok), BF), pltpu.VMEM((hd, q_group * tok), BF),
            pltpu.VMEM((2, n_chip, tok, chunk), F32),
            pltpu.VMEM((n_chip, q_group * tok, chunk), BF), pltpu.VMEM((n_chip, q_group * tok, chunk), BF),
            pltpu.VMEM((2, 2, n_chip, 2, hd, tok), F32), pltpu.VMEM((kv_heads, n_chip, 2, hd, tok), F32),
            pltpu.VMEM((kv_heads, 2, 2 * far - 1, hd, tok), F32),
            pltpu.VMEM((tok, width), F32), pltpu.VMEM((tok, width), F32),
            pltpu.VMEM((2, kv_heads, hd, tok), BF), pltpu.VMEM((kv_heads, hd, tok), BF),
            dma((2,)), dma((2 * n_chip,)), dma((2, 2)),
            dma((kv_heads,)), dma((kv_heads, 4 * far + 1)),
            dma((kv_heads,)), dma((kv_heads, n_chip)),
            dma((kv_heads,)), dma((kv_heads, 2, 2 * far - 1)),
            dma((kv_heads,)), dma((kv_heads,)), dma((width // gcol,)),
        ]
        out = jax.ShapeDtypeStruct((tok, width), BF)
        y, dx = pl.pallas_call(
            functools.partial(layer_kernel, n_dev, kv_heads, q_group),
            out_shape=(out, out),
            in_specs=[any_spec] * 6,
            out_specs=(any_spec, any_spec),
            scratch_shapes=scratch,
            name="layer",
            compiler_params=pltpu.CompilerParams(collective_id=0, has_side_effects=True,
                                                 vmem_limit_bytes=67043328),
        )(x_loc, dy_loc, w_q, w_k, w_v, w_o)
        n_part = 2
        return pl.pallas_call(
            store_kernel,
            out_shape=(out, out),
            in_specs=[any_spec] * 2,
            out_specs=(any_spec, any_spec),
            scratch_shapes=[pltpu.VMEM((2 * n_part, tok // n_part, width), BF),
                            dma((2 * n_part,)), dma((2 * n_part,))],
            name="store",
        )(y, dx)

    return jax.shard_map(local_body, mesh=mesh,
                         in_specs=(row_spec, row_spec, full_spec, full_spec, full_spec, full_spec),
                         out_specs=(row_spec, row_spec), check_vma=False)
```

```python
import functools
import math

import jax
import jax.numpy as jnp
from jax import lax
from jax.experimental import pallas as pl
from jax.experimental.pallas import tpu as pltpu
from jax.sharding import PartitionSpec as P

HEAD_DIM = 128
MESH = pl.DeviceIdType.MESH
BF = jnp.bfloat16
F32 = jnp.float32
UP, DOWN = 0, 1


def mm(a, b):
    return jnp.dot(a, b, preferred_element_type=F32)


def mm_nt(a, b):
    return lax.dot_general(a, b, (((1,), (1,)), ((), ())), preferred_element_type=F32)


def layer_kernel(n_dev, kv_heads, q_group,
                 x_hbm, dy_hbm, wq_hbm, wk_hbm, wv_hbm, wo_hbm, y_hbm, dx_hbm,
                 x_v, dy_v, wq_v, wo_v, kv_v, kt_v, vt_v, q_v, do_v, qt_v, dot_v,
                 s_v, p_v, ds_v, part_v, pre_v, ring_v, yacc_v, dxacc_v, fin_v, fout_v,
                 in_sem, w_sem, slab_sem, ag_send, ag_recv, pre_send, pre_recv, rs_send, rs_recv,
                 fin_send, fin_recv, out_sem):
    n_chip = n_dev // 2
    far = n_chip // 2
    tok = x_v.shape[0]
    width = x_v.shape[1]
    hd = HEAD_DIM
    gcol = q_group * hd
    kvcol = kv_heads * hd
    n_piece = width // gcol
    n_key = n_dev * tok
    chunk = 2 * tok
    scale = hd ** -0.5
    scale2 = scale * math.log2(math.e)

    me = lax.axis_index("cp")
    core = lax.rem(me, 2)
    chip = me // 2
    mate = me + 1 - 2 * core

    def chip_at(off):
        return lax.rem(chip + off + n_chip, n_chip)

    near = (2 * chip_at(1) + core, 2 * chip_at(-1) + core)
    next_near = (2 * chip_at(2) + core, 2 * chip_at(-2) + core)

    def remote(src, dst, ssem, rsem, dev):
        return pltpu.make_async_remote_copy(src_ref=src, dst_ref=dst, send_sem=ssem, recv_sem=rsem,
                                            device_id={"cp": dev}, device_id_type=MESH)

    def small_copies(hbm, buf, base):
        return [pltpu.make_async_copy(hbm.at[pl.ds((i // 2) * gcol, gcol), pl.ds((i % 2) * chunk, chunk)],
                                      buf.at[i], w_sem.at[base + i]) for i in range(n_chip)]

    def col_of(h):
        return h * gcol if isinstance(h, int) else pl.multiple_of(h * gcol, 128)

    def slab_q(h, slot):
        return pltpu.make_async_copy(wq_hbm.at[:, pl.ds(col_of(h), gcol)], wq_v.at[slot], slab_sem.at[slot, 0])

    def slab_o(h, slot):
        return pltpu.make_async_copy(wo_hbm.at[pl.ds(col_of(h), gcol), :], wo_v.at[slot], slab_sem.at[slot, 1])

    def src_chip(d, hop):
        return chip_at(-hop) if d == UP else chip_at(hop)

    def ag_view(h, dev, d, hop):
        if hop < far:
            return kv_v.at[h, dev]
        return kv_v.at[h, dev, d]

    def ag_ring(h, d, hop):
        ref = ag_view(h, 2 * src_chip(d, hop) + core, d, hop)
        return remote(ref, ref, ag_send.at[h], ag_recv.at[h, d * far + hop - 1], near[d])

    def ag_ring_out(h, d, hop, step=1):
        dev = me if hop == step else 2 * src_chip(d, hop - step) + core
        ref = ag_view(h, dev, d, hop)
        return remote(ref, ref, ag_send.at[h], ag_recv.at[h, d * far + hop - 1], (near if step == 1 else next_near)[d])

    def ag_mate_own(h):
        ref = kv_v.at[h, me]
        return remote(ref, ref, ag_send.at[h], ag_recv.at[h, 2 * far], mate)

    def ag_mate_out(h, d, hop):
        ref = ag_view(h, 2 * src_chip(d, hop) + core, d, hop)
        idx = 2 * far + 1 + d * far + hop - 1
        return remote(ref, ref, ag_send.at[h], ag_recv.at[h, idx], mate)

    def ag_mate_in(h, d, hop):
        ref = ag_view(h, 2 * src_chip(d, hop) + 1 - core, d, hop)
        idx = 2 * far + 1 + d * far + hop - 1
        return remote(ref, ref, ag_send.at[h], ag_recv.at[h, idx], mate)

    def ag_start(h, two=False):
        for d in (UP, DOWN):
            if two:
                ag_ring_out(h, d, 2, 2).start()
            ag_ring_out(h, d, 1).start()
        ag_mate_own(h).start()

    def ag_level(h, hop, two=False):
        for d in (UP, DOWN):
            ag_ring(h, d, hop).wait_recv()
            if two and hop == 2:
                ag_ring_out(h, d, 3).start()
                ag_ring_out(h, d, 4, 2).start()
            elif hop < far and not two:
                ag_ring_out(h, d, hop + 1).start()
            ag_mate_out(h, d, hop).start()

    def ag_finish(h):
        ref = kv_v.at[h, mate]
        remote(ref, ref, ag_send.at[h], ag_recv.at[h, 2 * far], mate).wait_recv()
        for hop in range(1, far + 1):
            for d in (UP, DOWN):
                ag_mate_in(h, d, hop).wait_recv()

    def ag_drain(h):
        ref = kv_v.at[h, pl.ds(0, n_dev - 1)]
        remote(ref, ref, ag_send.at[h], ag_recv.at[h, 0], mate).wait_send()

    def slot_of(off):
        return off % n_chip

    def pre_copy(h, off):
        slot, i = lax.rem(h, 2), slot_of(off)
        return remote(part_v.at[slot, 1 - core, i], pre_v.at[h, i], pre_send.at[h], pre_recv.at[h, i], mate)

    def chain_len(ch):
        return far - ch

    def rs_index(ch, lvl):
        return lvl if ch == 0 else far + lvl

    def rs_place(d, ch, lvl):
        dist = chain_len(ch) - lvl
        return slot_of(dist if d == UP else -dist), (ch if d == UP else 1 - ch)

    def rs_copy(h, d, ch, lvl):
        i = rs_index(ch, lvl)
        if lvl == 0:
            off, half = rs_place(d, ch, 0)
            src = part_v.at[lax.rem(h, 2), core, off, half]
        else:
            src = ring_v.at[h, d, rs_index(ch, lvl - 1)]
        return remote(src, ring_v.at[h, d, i], rs_send.at[h], rs_recv.at[h, d, i], near[d])

    def rs_begin(h):
        slot = lax.rem(h, 2)
        for off in (far, far - 1, 1 - far):
            pre_copy(h, off).wait_recv()
        for ch in (0, 1):
            for d in (UP, DOWN):
                off, half = rs_place(d, ch, 0)
                part_v[slot, core, off, half] = part_v[slot, core, off, half] + pre_v[h, off, half]
                rs_copy(h, d, ch, 0).start()

    def rs_step(h, ch, lvl):
        slot = lax.rem(h, 2)
        places = [rs_place(d, ch, lvl) for d in (UP, DOWN)]
        if ch == 1:
            for off, _ in places:
                pre_copy(h, off).wait_recv()
        mine = [part_v[slot, core, off, half] + pre_v[h, off, half] for off, half in places]
        i = rs_index(ch, lvl - 1)
        for d in (UP, DOWN):
            rs_copy(h, d, ch, lvl - 1).wait_recv()
            ring_v[h, d, i] = ring_v[h, d, i] + mine[d]
            rs_copy(h, d, ch, lvl).start()

    def fin_copy(h):
        return remote(fout_v.at[h], fin_v.at[core, h], fin_send.at[h], fin_recv.at[h], mate)

    def rs_end(h):
        slot = lax.rem(h, 2)
        pre_copy(h, 0).wait_recv()
        for ch in (0, 1):
            for d in (UP, DOWN):
                rs_copy(h, d, ch, chain_len(ch) - 1).wait_recv()
        factor = jnp.where(core == 0, scale, 1.0).astype(F32)
        for half in (0, 1):
            up = ring_v[h, UP, rs_index(half, chain_len(half) - 1)]
            dn = ring_v[h, DOWN, rs_index(1 - half, chain_len(1 - half) - 1)]
            total = (part_v[slot, core, 0, half] + pre_v[h, 0, half] + up + dn) * factor
            done = total.astype(BF)

            @pl.when(core == half)
            def _():
                fin_v[core, h] = done

            @pl.when(core != half)
            def _():
                fout_v[h] = done
        fin_copy(h).start()
        remote(ring_v.at[h], ring_v.at[h], rs_send.at[h], rs_recv.at[h, 0, 0], near[UP]).wait_send()
        remote(pre_v.at[h], pre_v.at[h], pre_send.at[h], pre_recv.at[h, 0], mate).wait_send()

    def project_q(h, slot):
        q_v[h] = mm(x_v[...], wq_v[slot]).astype(BF)

    do_cut = (gcol // 2 + chunk - 1) // chunk * chunk

    def project_do(h, slot, part=None):
        cols = {None: slice(0, gcol), 0: slice(0, do_cut), 1: slice(do_cut, gcol)}[part]
        do_v[h, :, cols] = mm_nt(dy_v[...], wo_v[slot, cols, :]).astype(BF)

    def transpose_kv(h):
        for e in range(n_dev):
            c, cols = e // 2, slice((e % 2) * tok, (e % 2 + 1) * tok)
            kt_v[c, :, cols] = kv_v[h, e, 0].T
            vt_v[c, :, cols] = kv_v[h, e, 1].T

    blk = 16
    n_blk = tok // blk

    def attend(h, serve):
        row_max, delta = {}, {}

        def lanes(j):
            return slice(j * hd, (j + 1) * hd)

        def rows(j):
            return slice(j * tok, (j + 1) * tok)

        def scores(j, i, state):
            if i == 0:
                qt_v[:, lanes(j)] = q_v[h, :, lanes(j)].T
                dot_v[:, lanes(j)] = do_v[h, :, lanes(j)].T
            s = mm(q_v[h, :, lanes(j)], kt_v[i]) * scale2
            s_v[j % 2, i] = s
            top = jnp.maximum(s[:, :hd], s[:, hd:])
            state["top"] = top if i == 0 else jnp.maximum(state["top"], top)
            if i == n_chip - 1:
                row_max[j] = jnp.max(state["top"], axis=1, keepdims=True)

        def exps(j, i, state):
            r = slice(i * blk, (i + 1) * blk)
            total = None
            for c in range(n_chip):
                e = jnp.exp2(s_v[j % 2, c, r, :] - row_max[j][r])
                s_v[j % 2, c, r, :] = e
                both = e[:, :hd] + e[:, hd:]
                total = both if total is None else total + both
            state[i] = 1.0 / jnp.sum(total, axis=1, keepdims=True)

        def probs(j, i, state):
            r = slice(i * blk, (i + 1) * blk)
            for c in range(n_chip):
                p_v[c, j * tok + i * blk:j * tok + (i + 1) * blk, :] = (s_v[j % 2, c, r, :] * state[i]).astype(BF)

        def kv_chunk(i, which):
            return kv_v[h, 2 * i:2 * i + 2, which].reshape(chunk, hd)

        def add_to(state, name, term):
            state[name] = term if name not in state else state[name] + term

        for b in range(-2, q_group + 1):
            state = {}
            soft = {}
            serve(b)
            for i in range(n_chip + 1):
                if i < n_chip and 0 <= b - 1 < q_group:
                    add_to(state, "dq", mm(ds_v[i, rows(b - 1), :], kv_chunk(i, 0)))
                if i < n_chip and 0 <= b + 2 < q_group:
                    scores(b + 2, i, state)
                if 0 <= b + 1 < q_group:
                    if i < n_blk:
                        exps(b + 1, i, soft)
                    if i > 0:
                        probs(b + 1, i - 1, soft)
            if 0 <= b - 1 < q_group:
                do_v[h, :, lanes(b - 1)] = (state["dq"] * scale).astype(BF)
            for i in range(n_chip):
                if 0 <= b + 1 < q_group:
                    add_to(state, "out", mm(p_v[i, rows(b + 1), :], kv_chunk(i, 1)))
                if 0 <= b < q_group:
                    dp = mm(do_v[h, :, lanes(b)], vt_v[i])
                    ds_v[i, rows(b), :] = (p_v[i, rows(b), :].astype(F32) * (dp - delta[b])).astype(BF)
            if 0 <= b + 1 < q_group:
                out = state["out"].astype(BF)
                q_v[h, :, lanes(b + 1)] = out
                do_j = do_v[h, :, lanes(b + 1)].astype(F32)
                delta[b + 1] = jnp.sum(out.astype(F32) * do_j, axis=1, keepdims=True)

    def key_grads(h):
        slot = lax.rem(h, 2)
        order = [far]
        for dist in range(far - 1, 0, -1):
            order += [dist, -dist]
        order.append(0)
        for group in (order[:3], order[3:]):
            for off in group:
                c = chip_at(off)
                gk = mm(qt_v[...], ds_v[c])
                gv = mm(dot_v[...], p_v[c])
                for half in (0, 1):
                    part_v[slot, 0, slot_of(off), half] = gk[:, half * tok:(half + 1) * tok]
                    part_v[slot, 1, slot_of(off), half] = gv[:, half * tok:(half + 1) * tok]
            for off in group:
                pre_copy(h, off).start()

    def outputs_y(h, slot):
        for b in range(n_piece):
            cols = slice(b * gcol, (b + 1) * gcol)
            yacc_v[:, cols] += mm(q_v[h], wo_v[slot, :, cols])

    def outputs_dx(h, slot):
        for b in range(n_piece):
            cols = slice(b * gcol, (b + 1) * gcol)
            dxacc_v[:, cols] += mm_nt(do_v[h], wq_v[slot, cols, :])

    x_copy = pltpu.make_async_copy(x_hbm, x_v, in_sem.at[0])
    dy_copy = pltpu.make_async_copy(dy_hbm, dy_v, in_sem.at[1])
    x_copy.start()
    wk_in = small_copies(wk_hbm, p_v, 0)
    wv_in = small_copies(wv_hbm, ds_v, n_chip)
    for copy in wk_in:
        copy.start()

    barrier = pltpu.get_barrier_semaphore()
    for dev in near + next_near + (mate,):
        pl.semaphore_signal(barrier, inc=1, device_id={"cp": dev}, device_id_type=MESH)

    yacc_v[...] = jnp.zeros_like(yacc_v)
    dxacc_v[...] = jnp.zeros_like(dxacc_v)
    for copy in wv_in:
        copy.start()
    x_copy.wait()

    def project_small(buf, which):
        acc = [None, None]
        for i in range(n_chip):
            b, half = i // 2, i % 2
            term = mm(x_v[:, b * gcol:(b + 1) * gcol], buf[i])
            acc[half] = term if b == 0 else acc[half] + term
        for h in range(kv_heads):
            col = (h % 2) * hd
            kv_v[h, me, which] = acc[h // 2][:, col:col + hd].astype(BF)

    for copy in wk_in:
        copy.wait()
    slab_q(2, 0).start()
    project_small(p_v, 0)
    for copy in wv_in:
        copy.wait()
    dy_copy.start()
    project_small(ds_v, 1)
    slab_o(2, 0).start()
    pl.semaphore_wait(barrier, 5)
    ag_start(0, True)

    slab_q(2, 0).wait()
    slab_q(1, 1).start()
    project_q(2, 0)
    slab_o(1, 1).start()
    dy_copy.wait()
    slab_o(2, 0).wait()
    slab_q(0, 0).start()
    project_do(2, 0)
    slab_o(0, 0).start()
    slab_q(1, 1).wait()
    project_q(1, 1)
    ag_level(0, 2, True)
    ag_level(0, 1, True)
    ag_start(1, True)
    slab_o(1, 1).wait()
    project_do(1, 1)
    slab_q(0, 0).wait()
    project_q(0, 0)
    ag_level(0, 3, True)
    slab_o(0, 0).wait()
    project_do(0, 0)
    ag_level(0, 4, True)

    first_serve = {-2: [(1, 2)], 1: [(1, 1)], 4: [(1, 3)], 6: [(1, 4)], 7: [(2, 1)]}

    def head_step(h, carry):
        def serve(b):
            if b in first_serve:
                @pl.when(h == 0)
                def _():
                    for g, hop in first_serve[b]:
                        ag_level(g, hop, g < 2)
                    if b in (1, 4):
                        ag_start(2 if b == 1 else 3)
            if b in (-1, 2, 5, 7):
                @pl.when(h == 1)
                def _():
                    if b == -1:
                        rs_step(h - 1, 0, 1)
                    elif b == 2:
                        rs_step(h - 1, 1, 1)
                        ag_level(2, 3)
                    elif b == 5:
                        rs_step(h - 1, 0, 2)
                        ag_level(3, 3)
                    else:
                        rs_step(h - 1, 1, 2)
            if b in (1, 5, 6, 7):
                @pl.when(h == 2)
                def _():
                    if b == 1:
                        ag_level(3, 4)
                    elif b == 5:
                        rs_step(h - 1, 0, 1)
                    elif b == 6:
                        rs_step(h - 1, 1, 1)
                    else:
                        rs_end(h - 2)
            if b in (0, 1, 3, 6, 7):
                @pl.when(h == 3)
                def _():
                    if b == 0:
                        rs_step(h - 2, 0, 3)
                    elif b == 1:
                        rs_step(h - 1, 0, 1)
                    elif b == 3:
                        rs_step(h - 1, 1, 1)
                    elif b == 6:
                        rs_step(h - 1, 0, 2)
                    else:
                        rs_end(h - 2)

        ag_finish(h)
        transpose_kv(h)
        attend(h, serve)
        key_grads(h)

        @pl.when(h == 1)
        def _():
            ag_level(2, 4)
            rs_step(h - 1, 0, 3)

        rs_begin(h)

        @pl.when(h == 0)
        def _():
            ag_level(3, 1)
            outputs_y(h, 0)
            slab_o(3, 0).start()
            ag_level(2, 2)
            outputs_dx(h, 0)
            slab_q(3, 0).start()
            ag_level(3, 2)

        @pl.when(h == 2)
        def _():
            slab_q(3, 0).wait()
            project_q(3, 0)
            rs_step(h - 1, 0, 2)
            rs_step(h - 1, 1, 2)
            slab_o(3, 0).wait()
            project_do(3, 0)

        return carry

    lax.fori_loop(0, kv_heads, head_step, 0)

    last = kv_heads - 1
    wk_in = small_copies(wk_hbm, p_v, 0)
    wv_in = small_copies(wv_hbm, ds_v, n_chip)
    for copy in wk_in + wv_in:
        copy.start()

    def fin_wait(h):
        remote(fout_v.at[h], fin_v.at[1 - core, h], fin_send.at[h], fin_recv.at[h], mate).wait_recv()

    def dx_copy(b):
        cols = pl.ds(b * gcol, gcol)
        return pltpu.make_async_copy(dy_v.at[:, cols], dx_hbm.at[:, cols], out_sem.at[b])

    def key_outputs(half, store):
        pair = (2 * half, 2 * half + 1)
        gk = jnp.concatenate([fin_v[0, h].T for h in pair], axis=1)
        gv = jnp.concatenate([fin_v[1, h].T for h in pair], axis=1)
        for b in range(n_piece):
            cols = slice(b * gcol, (b + 1) * gcol)
            i = 2 * b + half
            total = dxacc_v[:, cols] + mm_nt(gk, p_v[i]) + mm_nt(gv, ds_v[i])
            if store:
                dy_v[:, cols] = total.astype(BF)
                dx_copy(b).start()
            else:
                dxacc_v[:, cols] = total

    rs_step(2, 1, 2)
    outputs_y(1, 1)
    rs_step(2, 0, 3)
    slab_o(2, 1).start()
    outputs_dx(1, 1)
    slab_q(2, 1).start()
    rs_step(3, 0, 1)
    outputs_y(3, 0)
    rs_step(3, 1, 1)
    outputs_dx(3, 0)
    rs_end(2)
    rs_step(3, 0, 2)
    slab_o(2, 1).wait()
    outputs_y(2, 1)
    x_v[...] = yacc_v[...].astype(BF)
    y_copy = pltpu.make_async_copy(x_v, y_hbm, in_sem.at[0])
    y_copy.start()
    rs_step(3, 1, 2)
    for copy in wk_in + wv_in:
        copy.wait()
    fin_wait(0)
    fin_wait(1)
    key_outputs(0, False)
    rs_step(3, 0, 3)
    slab_q(2, 1).wait()
    outputs_dx(2, 1)
    for h in range(kv_heads):
        ag_drain(h)
    rs_end(3)
    fin_wait(2)
    fin_wait(3)
    key_outputs(1, True)
    for h in range(kv_heads):
        fin_copy(h).wait_send()
    y_copy.wait()
    for b in range(n_piece):
        dx_copy(b).wait()


def store_kernel(y_in, dx_in, y_out, dx_out, buf, in_sem, out_sem):
    n_part, rows = buf.shape[0] // 2, buf.shape[1]
    pairs = []
    for i in range(2 * n_part):
        src, dst = ((y_in, y_out), (dx_in, dx_out))[i // n_part]
        at = pl.ds((i % n_part) * rows, rows)
        pairs.append((pltpu.make_async_copy(src.at[at], buf.at[i], in_sem.at[i]),
                      pltpu.make_async_copy(buf.at[i], dst.at[at], out_sem.at[i])))
    for take, _ in pairs:
        take.start()
    for take, give in pairs:
        take.wait()
        give.start()
    for _, give in pairs:
        give.wait()


def solution(mesh):
    n_dev = mesh.shape["cp"]
    row_spec = P(("dp", "cp"), None)
    full_spec = P(None, None)

    def local_body(x_loc, dy_loc, w_q, w_k, w_v, w_o):
        tok, width = x_loc.shape
        q_heads = w_q.shape[1] // HEAD_DIM
        kv_heads = w_k.shape[1] // HEAD_DIM
        q_group = q_heads // kv_heads
        gcol = q_group * HEAD_DIM
        n_chip = n_dev // 2
        far = n_chip // 2
        chunk = 2 * tok
        hd = HEAD_DIM
        any_spec = pl.BlockSpec(memory_space=pl.ANY)
        dma = pltpu.SemaphoreType.DMA
        scratch = [
            pltpu.VMEM((tok, width), BF), pltpu.VMEM((tok, width), BF),
            pltpu.VMEM((2, width, gcol), BF), pltpu.VMEM((2, gcol, width), BF),
            pltpu.VMEM((kv_heads, n_dev, 2, tok, hd), BF),
            pltpu.VMEM((n_chip, hd, chunk), BF), pltpu.VMEM((n_chip, hd, chunk), BF),
            pltpu.VMEM((kv_heads, tok, gcol), BF), pltpu.VMEM((kv_heads, tok, gcol), BF),
            pltpu.VMEM((hd, q_group * tok), BF), pltpu.VMEM((hd, q_group * tok), BF),
            pltpu.VMEM((2, n_chip, tok, chunk), F32),
            pltpu.VMEM((n_chip, q_group * tok, chunk), BF), pltpu.VMEM((n_chip, q_group * tok, chunk), BF),
            pltpu.VMEM((2, 2, n_chip, 2, hd, tok), F32), pltpu.VMEM((kv_heads, n_chip, 2, hd, tok), F32),
            pltpu.VMEM((kv_heads, 2, 2 * far - 1, hd, tok), F32),
            pltpu.VMEM((tok, width), F32), pltpu.VMEM((tok, width), F32),
            pltpu.VMEM((2, kv_heads, hd, tok), BF), pltpu.VMEM((kv_heads, hd, tok), BF),
            dma((2,)), dma((2 * n_chip,)), dma((2, 2)),
            dma((kv_heads,)), dma((kv_heads, 4 * far + 1)),
            dma((kv_heads,)), dma((kv_heads, n_chip)),
            dma((kv_heads,)), dma((kv_heads, 2, 2 * far - 1)),
            dma((kv_heads,)), dma((kv_heads,)), dma((width // gcol,)),
        ]
        out = jax.ShapeDtypeStruct((tok, width), BF)
        y, dx = pl.pallas_call(
            functools.partial(layer_kernel, n_dev, kv_heads, q_group),
            out_shape=(out, out),
            in_specs=[any_spec] * 6,
            out_specs=(any_spec, any_spec),
            scratch_shapes=scratch,
            name="layer",
            compiler_params=pltpu.CompilerParams(collective_id=0, has_side_effects=True,
                                                 vmem_limit_bytes=67043328),
        )(x_loc, dy_loc, w_q, w_k, w_v, w_o)
        n_part = 2
        return pl.pallas_call(
            store_kernel,
            out_shape=(out, out),
            in_specs=[any_spec] * 2,
            out_specs=(any_spec, any_spec),
            scratch_shapes=[pltpu.VMEM((2 * n_part, tok // n_part, width), BF),
                            dma((2 * n_part,)), dma((2 * n_part,))],
            name="store",
        )(y, dx)

    return jax.shard_map(local_body, mesh=mesh,
                         in_specs=(row_spec, row_spec, full_spec, full_spec, full_spec, full_spec),
                         out_specs=(row_spec, row_spec), check_vma=False)
```

```python
import functools
import math

import jax
import jax.numpy as jnp
from jax import lax
from jax.experimental import pallas as pl
from jax.experimental.pallas import tpu as pltpu
from jax.sharding import PartitionSpec as P

HEAD_DIM = 128
MESH = pl.DeviceIdType.MESH
BF = jnp.bfloat16
F32 = jnp.float32
UP, DOWN = 0, 1


def mm(a, b):
    return jnp.dot(a, b, preferred_element_type=F32)


def mm_nt(a, b):
    return lax.dot_general(a, b, (((1,), (1,)), ((), ())), preferred_element_type=F32)


def layer_kernel(n_dev, kv_heads, q_group,
                 x_hbm, dy_hbm, wq_hbm, wk_hbm, wv_hbm, wo_hbm, y_hbm, dx_hbm,
                 x_v, dy_v, wq_v, wo_v, kv_v, kt_v, vt_v, q_v, do_v, qt_v, dot_v,
                 s_v, p_v, ds_v, part_v, pre_v, ring_v, yacc_v, dxacc_v, fin_v, fout_v,
                 in_sem, w_sem, slab_sem, ag_send, ag_recv, pre_send, pre_recv, rs_send, rs_recv,
                 fin_send, fin_recv, out_sem):
    n_chip = n_dev // 2
    far = n_chip // 2
    tok = x_v.shape[0]
    width = x_v.shape[1]
    hd = HEAD_DIM
    gcol = q_group * hd
    kvcol = kv_heads * hd
    n_piece = width // gcol
    n_key = n_dev * tok
    chunk = 2 * tok
    scale = hd ** -0.5
    scale2 = scale * math.log2(math.e)

    me = lax.axis_index("cp")
    core = lax.rem(me, 2)
    chip = me // 2
    mate = me + 1 - 2 * core

    def chip_at(off):
        return lax.rem(chip + off + n_chip, n_chip)

    near = (2 * chip_at(1) + core, 2 * chip_at(-1) + core)
    next_near = (2 * chip_at(2) + core, 2 * chip_at(-2) + core)

    def remote(src, dst, ssem, rsem, dev):
        return pltpu.make_async_remote_copy(src_ref=src, dst_ref=dst, send_sem=ssem, recv_sem=rsem,
                                            device_id={"cp": dev}, device_id_type=MESH)

    def small_copies(hbm, buf, base):
        return [pltpu.make_async_copy(hbm.at[pl.ds((i // 2) * gcol, gcol), pl.ds((i % 2) * chunk, chunk)],
                                      buf.at[i], w_sem.at[base + i]) for i in range(n_chip)]

    def col_of(h):
        return h * gcol if isinstance(h, int) else pl.multiple_of(h * gcol, 128)

    def slab_q(h, slot):
        return pltpu.make_async_copy(wq_hbm.at[:, pl.ds(col_of(h), gcol)], wq_v.at[slot], slab_sem.at[slot, 0])

    def slab_o(h, slot):
        return pltpu.make_async_copy(wo_hbm.at[pl.ds(col_of(h), gcol), :], wo_v.at[slot], slab_sem.at[slot, 1])

    def src_chip(d, hop):
        return chip_at(-hop) if d == UP else chip_at(hop)

    def ag_view(h, dev, d, hop):
        if hop < far:
            return kv_v.at[h, dev]
        return kv_v.at[h, dev, d]

    def ag_ring(h, d, hop):
        ref = ag_view(h, 2 * src_chip(d, hop) + core, d, hop)
        return remote(ref, ref, ag_send.at[h], ag_recv.at[h, d * far + hop - 1], near[d])

    def ag_ring_out(h, d, hop, step=1):
        dev = me if hop == step else 2 * src_chip(d, hop - step) + core
        ref = ag_view(h, dev, d, hop)
        return remote(ref, ref, ag_send.at[h], ag_recv.at[h, d * far + hop - 1], (near if step == 1 else next_near)[d])

    def ag_mate_own(h):
        ref = kv_v.at[h, me]
        return remote(ref, ref, ag_send.at[h], ag_recv.at[h, 2 * far], mate)

    def ag_mate_out(h, d, hop):
        ref = ag_view(h, 2 * src_chip(d, hop) + core, d, hop)
        idx = 2 * far + 1 + d * far + hop - 1
        return remote(ref, ref, ag_send.at[h], ag_recv.at[h, idx], mate)

    def ag_mate_in(h, d, hop):
        ref = ag_view(h, 2 * src_chip(d, hop) + 1 - core, d, hop)
        idx = 2 * far + 1 + d * far + hop - 1
        return remote(ref, ref, ag_send.at[h], ag_recv.at[h, idx], mate)

    def ag_start(h, two=False):
        for d in (UP, DOWN):
            if two:
                ag_ring_out(h, d, 2, 2).start()
            ag_ring_out(h, d, 1).start()
        ag_mate_own(h).start()

    def ag_level(h, hop, two=False):
        for d in (UP, DOWN):
            ag_ring(h, d, hop).wait_recv()
            if two and hop == 2:
                ag_ring_out(h, d, 3).start()
                ag_ring_out(h, d, 4, 2).start()
            elif hop < far and not two:
                ag_ring_out(h, d, hop + 1).start()
            ag_mate_out(h, d, hop).start()

    def ag_finish(h):
        ref = kv_v.at[h, mate]
        remote(ref, ref, ag_send.at[h], ag_recv.at[h, 2 * far], mate).wait_recv()
        for hop in range(1, far + 1):
            for d in (UP, DOWN):
                ag_mate_in(h, d, hop).wait_recv()

    def ag_drain(h):
        ref = kv_v.at[h, pl.ds(0, n_dev - 1)]
        remote(ref, ref, ag_send.at[h], ag_recv.at[h, 0], mate).wait_send()

    def slot_of(off):
        return off % n_chip

    def pre_copy(h, off):
        slot, i = lax.rem(h, 2), slot_of(off)
        return remote(part_v.at[slot, 1 - core, i], pre_v.at[h, i], pre_send.at[h], pre_recv.at[h, i], mate)

    def chain_len(ch):
        return far - ch

    def rs_index(ch, lvl):
        return lvl if ch == 0 else far + lvl

    def rs_place(d, ch, lvl):
        dist = chain_len(ch) - lvl
        return slot_of(dist if d == UP else -dist), (ch if d == UP else 1 - ch)

    def rs_copy(h, d, ch, lvl):
        i = rs_index(ch, lvl)
        if lvl == 0:
            off, half = rs_place(d, ch, 0)
            src = part_v.at[lax.rem(h, 2), core, off, half]
        else:
            src = ring_v.at[h, d, rs_index(ch, lvl - 1)]
        return remote(src, ring_v.at[h, d, i], rs_send.at[h], rs_recv.at[h, d, i], near[d])

    def rs_begin(h):
        slot = lax.rem(h, 2)
        for off in (far, far - 1, 1 - far):
            pre_copy(h, off).wait_recv()
        for ch in (0, 1):
            for d in (UP, DOWN):
                off, half = rs_place(d, ch, 0)
                part_v[slot, core, off, half] = part_v[slot, core, off, half] + pre_v[h, off, half]
                rs_copy(h, d, ch, 0).start()

    def rs_step(h, ch, lvl):
        slot = lax.rem(h, 2)
        places = [rs_place(d, ch, lvl) for d in (UP, DOWN)]
        if ch == 1:
            for off, _ in places:
                pre_copy(h, off).wait_recv()
        mine = [part_v[slot, core, off, half] + pre_v[h, off, half] for off, half in places]
        i = rs_index(ch, lvl - 1)
        for d in (UP, DOWN):
            rs_copy(h, d, ch, lvl - 1).wait_recv()
            ring_v[h, d, i] = ring_v[h, d, i] + mine[d]
            rs_copy(h, d, ch, lvl).start()

    def fin_copy(h):
        return remote(fout_v.at[h], fin_v.at[core, h], fin_send.at[h], fin_recv.at[h], mate)

    def rs_end(h):
        slot = lax.rem(h, 2)
        pre_copy(h, 0).wait_recv()
        for ch in (0, 1):
            for d in (UP, DOWN):
                rs_copy(h, d, ch, chain_len(ch) - 1).wait_recv()
        factor = jnp.where(core == 0, scale, 1.0).astype(F32)
        for half in (0, 1):
            up = ring_v[h, UP, rs_index(half, chain_len(half) - 1)]
            dn = ring_v[h, DOWN, rs_index(1 - half, chain_len(1 - half) - 1)]
            total = (part_v[slot, core, 0, half] + pre_v[h, 0, half] + up + dn) * factor
            done = total.astype(BF)

            @pl.when(core == half)
            def _():
                fin_v[core, h] = done

            @pl.when(core != half)
            def _():
                fout_v[h] = done
        fin_copy(h).start()
        remote(ring_v.at[h], ring_v.at[h], rs_send.at[h], rs_recv.at[h, 0, 0], near[UP]).wait_send()
        remote(pre_v.at[h], pre_v.at[h], pre_send.at[h], pre_recv.at[h, 0], mate).wait_send()

    def project_q(h, slot):
        q_v[h] = mm(x_v[...], wq_v[slot]).astype(BF)

    do_cut = (gcol // 2 + chunk - 1) // chunk * chunk

    def project_do(h, slot, part=None):
        cols = {None: slice(0, gcol), 0: slice(0, do_cut), 1: slice(do_cut, gcol)}[part]
        do_v[h, :, cols] = mm_nt(dy_v[...], wo_v[slot, cols, :]).astype(BF)

    def transpose_kv(h):
        for e in range(n_dev):
            c, cols = e // 2, slice((e % 2) * tok, (e % 2 + 1) * tok)
            kt_v[c, :, cols] = kv_v[h, e, 0].T
            vt_v[c, :, cols] = kv_v[h, e, 1].T

    blk = 16
    n_blk = tok // blk

    def attend(h, serve):
        row_max, delta = {}, {}

        def lanes(j):
            return slice(j * hd, (j + 1) * hd)

        def rows(j):
            return slice(j * tok, (j + 1) * tok)

        def scores(j, i, state):
            if i == 0:
                qt_v[:, lanes(j)] = q_v[h, :, lanes(j)].T
                dot_v[:, lanes(j)] = do_v[h, :, lanes(j)].T
            s = mm(q_v[h, :, lanes(j)], kt_v[i]) * scale2
            s_v[j % 2, i] = s
            top = jnp.maximum(s[:, :hd], s[:, hd:])
            state["top"] = top if i == 0 else jnp.maximum(state["top"], top)
            if i == n_chip - 1:
                row_max[j] = jnp.max(state["top"], axis=1, keepdims=True)

        def exps(j, i, state):
            r = slice(i * blk, (i + 1) * blk)
            total = None
            for c in range(n_chip):
                e = jnp.exp2(s_v[j % 2, c, r, :] - row_max[j][r])
                s_v[j % 2, c, r, :] = e
                both = e[:, :hd] + e[:, hd:]
                total = both if total is None else total + both
            state[i] = 1.0 / jnp.sum(total, axis=1, keepdims=True)

        def probs(j, i, state):
            r = slice(i * blk, (i + 1) * blk)
            for c in range(n_chip):
                p_v[c, j * tok + i * blk:j * tok + (i + 1) * blk, :] = (s_v[j % 2, c, r, :] * state[i]).astype(BF)

        def kv_chunk(i, which):
            return kv_v[h, 2 * i:2 * i + 2, which].reshape(chunk, hd)

        def add_to(state, name, term):
            state[name] = term if name not in state else state[name] + term

        for b in range(-2, q_group + 1):
            state = {}
            soft = {}
            serve(b)
            for i in range(n_chip + 1):
                if i < n_chip and 0 <= b - 1 < q_group:
                    add_to(state, "dq", mm(ds_v[i, rows(b - 1), :], kv_chunk(i, 0)))
                if i < n_chip and 0 <= b + 2 < q_group:
                    scores(b + 2, i, state)
                if 0 <= b + 1 < q_group:
                    if i < n_blk:
                        exps(b + 1, i, soft)
                    if i > 0:
                        probs(b + 1, i - 1, soft)
            if 0 <= b - 1 < q_group:
                do_v[h, :, lanes(b - 1)] = (state["dq"] * scale).astype(BF)
            for i in range(n_chip):
                if 0 <= b + 1 < q_group:
                    add_to(state, "out", mm(p_v[i, rows(b + 1), :], kv_chunk(i, 1)))
                if 0 <= b < q_group:
                    dp = mm(do_v[h, :, lanes(b)], vt_v[i])
                    ds_v[i, rows(b), :] = (p_v[i, rows(b), :].astype(F32) * (dp - delta[b])).astype(BF)
            if 0 <= b + 1 < q_group:
                out = state["out"].astype(BF)
                q_v[h, :, lanes(b + 1)] = out
                do_j = do_v[h, :, lanes(b + 1)].astype(F32)
                delta[b + 1] = jnp.sum(out.astype(F32) * do_j, axis=1, keepdims=True)

    def key_grads(h):
        slot = lax.rem(h, 2)
        order = [far]
        for dist in range(far - 1, 0, -1):
            order += [dist, -dist]
        order.append(0)
        for group in (order[:3], order[3:]):
            for off in group:
                c = chip_at(off)
                gk = mm(qt_v[...], ds_v[c])
                gv = mm(dot_v[...], p_v[c])
                for half in (0, 1):
                    part_v[slot, 0, slot_of(off), half] = gk[:, half * tok:(half + 1) * tok]
                    part_v[slot, 1, slot_of(off), half] = gv[:, half * tok:(half + 1) * tok]
            for off in group:
                pre_copy(h, off).start()

    def outputs_y(h, slot):
        for b in range(n_piece):
            cols = slice(b * gcol, (b + 1) * gcol)
            yacc_v[:, cols] += mm(q_v[h], wo_v[slot, :, cols])

    def outputs_dx(h, slot):
        for b in range(n_piece):
            cols = slice(b * gcol, (b + 1) * gcol)
            dxacc_v[:, cols] += mm_nt(do_v[h], wq_v[slot, cols, :])

    x_copy = pltpu.make_async_copy(x_hbm, x_v, in_sem.at[0])
    dy_copy = pltpu.make_async_copy(dy_hbm, dy_v, in_sem.at[1])
    x_copy.start()
    wk_in = small_copies(wk_hbm, p_v, 0)
    wv_in = small_copies(wv_hbm, ds_v, n_chip)
    for copy in wk_in:
        copy.start()

    barrier = pltpu.get_barrier_semaphore()
    for dev in near + next_near + (mate,):
        pl.semaphore_signal(barrier, inc=1, device_id={"cp": dev}, device_id_type=MESH)

    yacc_v[...] = jnp.zeros_like(yacc_v)
    dxacc_v[...] = jnp.zeros_like(dxacc_v)
    for copy in wv_in:
        copy.start()
    x_copy.wait()

    def project_small(buf, which):
        acc = [None, None]
        for i in range(n_chip):
            b, half = i // 2, i % 2
            term = mm(x_v[:, b * gcol:(b + 1) * gcol], buf[i])
            acc[half] = term if b == 0 else acc[half] + term
        for h in range(kv_heads):
            col = (h % 2) * hd
            kv_v[h, me, which] = acc[h // 2][:, col:col + hd].astype(BF)

    for copy in wk_in:
        copy.wait()
    slab_q(2, 0).start()
    project_small(p_v, 0)
    for copy in wv_in:
        copy.wait()
    dy_copy.start()
    project_small(ds_v, 1)
    slab_o(2, 0).start()
    pl.semaphore_wait(barrier, 5)
    ag_start(0, True)

    slab_q(2, 0).wait()
    slab_q(1, 1).start()
    project_q(2, 0)
    slab_o(1, 1).start()
    dy_copy.wait()
    slab_o(2, 0).wait()
    slab_q(0, 0).start()
    project_do(2, 0)
    slab_o(0, 0).start()
    slab_q(1, 1).wait()
    project_q(1, 1)
    ag_level(0, 2, True)
    ag_level(0, 1, True)
    ag_start(1, True)
    slab_o(1, 1).wait()
    project_do(1, 1)
    slab_q(0, 0).wait()
    project_q(0, 0)
    ag_level(0, 3, True)
    slab_o(0, 0).wait()
    project_do(0, 0)
    ag_level(0, 4, True)

    first_serve = {-2: [(1, 2)], 1: [(1, 1)], 4: [(1, 3)], 6: [(1, 4)], 7: [(2, 1)]}

    def head_step(h, carry):
        def serve(b):
            if b in first_serve:
                @pl.when(h == 0)
                def _():
                    for g, hop in first_serve[b]:
                        ag_level(g, hop, g < 2)
                    if b in (1, 4):
                        ag_start(2 if b == 1 else 3)
            if b in (-1, 2, 4, 5, 7):
                @pl.when(h == 1)
                def _():
                    if b == -1:
                        rs_step(h - 1, 0, 1)
                    elif b == 2:
                        rs_step(h - 1, 1, 1)
                    elif b == 4:
                        ag_level(2, 3)
                    elif b == 5:
                        rs_step(h - 1, 0, 2)
                    else:
                        rs_step(h - 1, 1, 2)
                        ag_level(2, 4)
                        ag_level(3, 2)
            if b in (1, 5, 6, 7):
                @pl.when(h == 2)
                def _():
                    if b == 1:
                        ag_level(3, 3)
                    elif b == 5:
                        rs_step(h - 1, 0, 1)
                    elif b == 6:
                        rs_step(h - 1, 1, 1)
                    else:
                        rs_end(h - 2)
                        ag_level(3, 4)
            if b in (1, 3, 7):
                @pl.when(h == 3)
                def _():
                    if b == 1:
                        rs_step(h - 2, 0, 3)
                        rs_step(h - 1, 0, 1)
                    elif b == 3:
                        rs_step(h - 1, 1, 1)
                    else:
                        rs_step(h - 1, 0, 2)
                        rs_end(h - 2)

        ag_finish(h)
        transpose_kv(h)
        attend(h, serve)
        key_grads(h)

        @pl.when(h == 1)
        def _():
            rs_step(h - 1, 0, 3)

        @pl.when(h == 2)
        def _():
            slab_q(3, 0).wait()
            project_q(3, 0)
            rs_step(h - 1, 0, 2)

        @pl.when(h == 0)
        def _():
            outputs_y(h, 0)
            slab_o(3, 0).start()

        rs_begin(h)

        @pl.when(h == 0)
        def _():
            ag_level(3, 1)
            ag_level(2, 2)
            outputs_dx(h, 0)
            slab_q(3, 0).start()

        @pl.when(h == 2)
        def _():
            rs_step(h - 1, 1, 2)
            slab_o(3, 0).wait()
            project_do(3, 0)

        return carry

    lax.fori_loop(0, kv_heads, head_step, 0)

    last = kv_heads - 1
    wk_in = small_copies(wk_hbm, p_v, 0)
    wv_in = small_copies(wv_hbm, ds_v, n_chip)
    for copy in wk_in + wv_in:
        copy.start()

    def fin_wait(h):
        remote(fout_v.at[h], fin_v.at[1 - core, h], fin_send.at[h], fin_recv.at[h], mate).wait_recv()

    def dx_copy(b):
        cols = pl.ds(b * gcol, gcol)
        return pltpu.make_async_copy(dy_v.at[:, cols], dx_hbm.at[:, cols], out_sem.at[b])

    def key_outputs(half, store):
        pair = (2 * half, 2 * half + 1)
        gk = jnp.concatenate([fin_v[0, h].T for h in pair], axis=1)
        gv = jnp.concatenate([fin_v[1, h].T for h in pair], axis=1)
        for b in range(n_piece):
            cols = slice(b * gcol, (b + 1) * gcol)
            i = 2 * b + half
            total = dxacc_v[:, cols] + mm_nt(gk, p_v[i]) + mm_nt(gv, ds_v[i])
            if store:
                dy_v[:, cols] = total.astype(BF)
                dx_copy(b).start()
            else:
                dxacc_v[:, cols] = total

    rs_step(2, 1, 2)
    outputs_y(1, 1)
    rs_step(2, 0, 3)
    slab_o(2, 1).start()
    outputs_dx(1, 1)
    slab_q(2, 1).start()
    rs_step(3, 0, 1)
    outputs_y(3, 0)
    rs_step(3, 1, 1)
    outputs_dx(3, 0)
    rs_end(2)
    rs_step(3, 0, 2)
    slab_o(2, 1).wait()
    outputs_y(2, 1)
    x_v[...] = yacc_v[...].astype(BF)
    y_copy = pltpu.make_async_copy(x_v, y_hbm, in_sem.at[0])
    y_copy.start()
    rs_step(3, 1, 2)
    for copy in wk_in + wv_in:
        copy.wait()
    fin_wait(0)
    fin_wait(1)
    key_outputs(0, False)
    rs_step(3, 0, 3)
    slab_q(2, 1).wait()
    outputs_dx(2, 1)
    for h in range(kv_heads):
        ag_drain(h)
    rs_end(3)
    fin_wait(2)
    fin_wait(3)
    key_outputs(1, True)
    for h in range(kv_heads):
        fin_copy(h).wait_send()
    y_copy.wait()
    for b in range(n_piece):
        dx_copy(b).wait()


def store_kernel(y_in, dx_in, y_out, dx_out, buf, in_sem, out_sem):
    n_part, rows = buf.shape[0] // 2, buf.shape[1]
    pairs = []
    for i in range(2 * n_part):
        src, dst = ((y_in, y_out), (dx_in, dx_out))[i // n_part]
        at = pl.ds((i % n_part) * rows, rows)
        pairs.append((pltpu.make_async_copy(src.at[at], buf.at[i], in_sem.at[i]),
                      pltpu.make_async_copy(buf.at[i], dst.at[at], out_sem.at[i])))
    for take, _ in pairs:
        take.start()
    for take, give in pairs:
        take.wait()
        give.start()
    for _, give in pairs:
        give.wait()


def solution(mesh):
    n_dev = mesh.shape["cp"]
    row_spec = P(("dp", "cp"), None)
    full_spec = P(None, None)

    def local_body(x_loc, dy_loc, w_q, w_k, w_v, w_o):
        tok, width = x_loc.shape
        q_heads = w_q.shape[1] // HEAD_DIM
        kv_heads = w_k.shape[1] // HEAD_DIM
        q_group = q_heads // kv_heads
        gcol = q_group * HEAD_DIM
        n_chip = n_dev // 2
        far = n_chip // 2
        chunk = 2 * tok
        hd = HEAD_DIM
        any_spec = pl.BlockSpec(memory_space=pl.ANY)
        dma = pltpu.SemaphoreType.DMA
        scratch = [
            pltpu.VMEM((tok, width), BF), pltpu.VMEM((tok, width), BF),
            pltpu.VMEM((2, width, gcol), BF), pltpu.VMEM((2, gcol, width), BF),
            pltpu.VMEM((kv_heads, n_dev, 2, tok, hd), BF),
            pltpu.VMEM((n_chip, hd, chunk), BF), pltpu.VMEM((n_chip, hd, chunk), BF),
            pltpu.VMEM((kv_heads, tok, gcol), BF), pltpu.VMEM((kv_heads, tok, gcol), BF),
            pltpu.VMEM((hd, q_group * tok), BF), pltpu.VMEM((hd, q_group * tok), BF),
            pltpu.VMEM((2, n_chip, tok, chunk), F32),
            pltpu.VMEM((n_chip, q_group * tok, chunk), BF), pltpu.VMEM((n_chip, q_group * tok, chunk), BF),
            pltpu.VMEM((2, 2, n_chip, 2, hd, tok), F32), pltpu.VMEM((kv_heads, n_chip, 2, hd, tok), F32),
            pltpu.VMEM((kv_heads, 2, 2 * far - 1, hd, tok), F32),
            pltpu.VMEM((tok, width), F32), pltpu.VMEM((tok, width), F32),
            pltpu.VMEM((2, kv_heads, hd, tok), BF), pltpu.VMEM((kv_heads, hd, tok), BF),
            dma((2,)), dma((2 * n_chip,)), dma((2, 2)),
            dma((kv_heads,)), dma((kv_heads, 4 * far + 1)),
            dma((kv_heads,)), dma((kv_heads, n_chip)),
            dma((kv_heads,)), dma((kv_heads, 2, 2 * far - 1)),
            dma((kv_heads,)), dma((kv_heads,)), dma((width // gcol,)),
        ]
        out = jax.ShapeDtypeStruct((tok, width), BF)
        y, dx = pl.pallas_call(
            functools.partial(layer_kernel, n_dev, kv_heads, q_group),
            out_shape=(out, out),
            in_specs=[any_spec] * 6,
            out_specs=(any_spec, any_spec),
            scratch_shapes=scratch,
            name="layer",
            compiler_params=pltpu.CompilerParams(collective_id=0, has_side_effects=True,
                                                 vmem_limit_bytes=67043328),
        )(x_loc, dy_loc, w_q, w_k, w_v, w_o)
        n_part = 2
        return pl.pallas_call(
            store_kernel,
            out_shape=(out, out),
            in_specs=[any_spec] * 2,
            out_specs=(any_spec, any_spec),
            scratch_shapes=[pltpu.VMEM((2 * n_part, tok // n_part, width), BF),
                            dma((2 * n_part,)), dma((2 * n_part,))],
            name="store",
        )(y, dx)

    return jax.shard_map(local_body, mesh=mesh,
                         in_specs=(row_spec, row_spec, full_spec, full_spec, full_spec, full_spec),
                         out_specs=(row_spec, row_spec), check_vma=False)
```

```python
import functools
import math

import jax
import jax.numpy as jnp
from jax import lax
from jax.experimental import pallas as pl
from jax.experimental.pallas import tpu as pltpu
from jax.sharding import PartitionSpec as P

HEAD_DIM = 128
MESH = pl.DeviceIdType.MESH
BF = jnp.bfloat16
F32 = jnp.float32
UP, DOWN = 0, 1


def mm(a, b):
    return jnp.dot(a, b, preferred_element_type=F32)


def mm_nt(a, b):
    return lax.dot_general(a, b, (((1,), (1,)), ((), ())), preferred_element_type=F32)


def layer_kernel(n_dev, kv_heads, q_group,
                 x_hbm, dy_hbm, wq_hbm, wk_hbm, wv_hbm, wo_hbm, y_hbm, dx_hbm,
                 x_v, dy_v, wq_v, wo_v, kv_v, kt_v, vt_v, q_v, do_v, qt_v, dot_v,
                 s_v, p_v, ds_v, part_v, pre_v, ring_v, yacc_v, dxacc_v, fin_v, fout_v,
                 in_sem, w_sem, slab_sem, ag_send, ag_recv, pre_send, pre_recv, rs_send, rs_recv,
                 fin_send, fin_recv, out_sem):
    n_chip = n_dev // 2
    far = n_chip // 2
    tok = x_v.shape[0]
    width = x_v.shape[1]
    hd = HEAD_DIM
    gcol = q_group * hd
    kvcol = kv_heads * hd
    n_piece = width // gcol
    n_key = n_dev * tok
    chunk = 2 * tok
    scale = hd ** -0.5
    scale2 = scale * math.log2(math.e)

    me = lax.axis_index("cp")
    core = lax.rem(me, 2)
    chip = me // 2
    mate = me + 1 - 2 * core

    def chip_at(off):
        return lax.rem(chip + off + n_chip, n_chip)

    near = (2 * chip_at(1) + core, 2 * chip_at(-1) + core)
    next_near = (2 * chip_at(2) + core, 2 * chip_at(-2) + core)

    def remote(src, dst, ssem, rsem, dev):
        return pltpu.make_async_remote_copy(src_ref=src, dst_ref=dst, send_sem=ssem, recv_sem=rsem,
                                            device_id={"cp": dev}, device_id_type=MESH)

    def small_copies(hbm, buf, base):
        return [pltpu.make_async_copy(hbm.at[pl.ds((i // 2) * gcol, gcol), pl.ds((i % 2) * chunk, chunk)],
                                      buf.at[i], w_sem.at[base + i]) for i in range(n_chip)]

    def col_of(h):
        return h * gcol if isinstance(h, int) else pl.multiple_of(h * gcol, 128)

    def slab_q(h, slot):
        return pltpu.make_async_copy(wq_hbm.at[:, pl.ds(col_of(h), gcol)], wq_v.at[slot], slab_sem.at[slot, 0])

    def slab_o(h, slot):
        return pltpu.make_async_copy(wo_hbm.at[pl.ds(col_of(h), gcol), :], wo_v.at[slot], slab_sem.at[slot, 1])

    def src_chip(d, hop):
        return chip_at(-hop) if d == UP else chip_at(hop)

    def ag_view(h, dev, d, hop):
        if hop < far:
            return kv_v.at[h, dev]
        return kv_v.at[h, dev, d]

    def ag_ring(h, d, hop):
        ref = ag_view(h, 2 * src_chip(d, hop) + core, d, hop)
        return remote(ref, ref, ag_send.at[h], ag_recv.at[h, d * far + hop - 1], near[d])

    def ag_ring_out(h, d, hop, step=1):
        dev = me if hop == step else 2 * src_chip(d, hop - step) + core
        ref = ag_view(h, dev, d, hop)
        return remote(ref, ref, ag_send.at[h], ag_recv.at[h, d * far + hop - 1], (near if step == 1 else next_near)[d])

    def ag_mate_own(h):
        ref = kv_v.at[h, me]
        return remote(ref, ref, ag_send.at[h], ag_recv.at[h, 2 * far], mate)

    def ag_mate_out(h, d, hop):
        ref = ag_view(h, 2 * src_chip(d, hop) + core, d, hop)
        idx = 2 * far + 1 + d * far + hop - 1
        return remote(ref, ref, ag_send.at[h], ag_recv.at[h, idx], mate)

    def ag_mate_in(h, d, hop):
        ref = ag_view(h, 2 * src_chip(d, hop) + 1 - core, d, hop)
        idx = 2 * far + 1 + d * far + hop - 1
        return remote(ref, ref, ag_send.at[h], ag_recv.at[h, idx], mate)

    def ag_start(h, two=False):
        for d in (UP, DOWN):
            if two:
                ag_ring_out(h, d, 2, 2).start()
            ag_ring_out(h, d, 1).start()
        ag_mate_own(h).start()

    def ag_level(h, hop, two=False):
        for d in (UP, DOWN):
            ag_ring(h, d, hop).wait_recv()
            if two and hop == 2:
                ag_ring_out(h, d, 3).start()
                ag_ring_out(h, d, 4, 2).start()
            elif hop < far and not two:
                ag_ring_out(h, d, hop + 1).start()
            ag_mate_out(h, d, hop).start()

    def ag_finish(h):
        ref = kv_v.at[h, mate]
        remote(ref, ref, ag_send.at[h], ag_recv.at[h, 2 * far], mate).wait_recv()
        for hop in range(1, far + 1):
            for d in (UP, DOWN):
                ag_mate_in(h, d, hop).wait_recv()

    def ag_drain(h):
        ref = kv_v.at[h, pl.ds(0, n_dev - 1)]
        remote(ref, ref, ag_send.at[h], ag_recv.at[h, 0], mate).wait_send()

    def slot_of(off):
        return off % n_chip

    def pre_copy(h, off):
        slot, i = lax.rem(h, 2), slot_of(off)
        return remote(part_v.at[slot, 1 - core, i], pre_v.at[h, i], pre_send.at[h], pre_recv.at[h, i], mate)

    def chain_len(ch):
        return far - ch

    def rs_index(ch, lvl):
        return lvl if ch == 0 else far + lvl

    def rs_place(d, ch, lvl):
        dist = chain_len(ch) - lvl
        return slot_of(dist if d == UP else -dist), (ch if d == UP else 1 - ch)

    def rs_copy(h, d, ch, lvl):
        i = rs_index(ch, lvl)
        if lvl == 0:
            off, half = rs_place(d, ch, 0)
            src = part_v.at[lax.rem(h, 2), core, off, half]
        else:
            src = ring_v.at[h, d, rs_index(ch, lvl - 1)]
        return remote(src, ring_v.at[h, d, i], rs_send.at[h], rs_recv.at[h, d, i], near[d])

    def rs_begin(h):
        slot = lax.rem(h, 2)
        for off in (far, far - 1, 1 - far):
            pre_copy(h, off).wait_recv()
        for ch in (0, 1):
            for d in (UP, DOWN):
                off, half = rs_place(d, ch, 0)
                part_v[slot, core, off, half] = part_v[slot, core, off, half] + pre_v[h, off, half]
                rs_copy(h, d, ch, 0).start()

    def rs_step(h, ch, lvl):
        slot = lax.rem(h, 2)
        places = [rs_place(d, ch, lvl) for d in (UP, DOWN)]
        if ch == 1:
            for off, _ in places:
                pre_copy(h, off).wait_recv()
        mine = [part_v[slot, core, off, half] + pre_v[h, off, half] for off, half in places]
        i = rs_index(ch, lvl - 1)
        for d in (UP, DOWN):
            rs_copy(h, d, ch, lvl - 1).wait_recv()
            ring_v[h, d, i] = ring_v[h, d, i] + mine[d]
            rs_copy(h, d, ch, lvl).start()

    def fin_copy(h):
        return remote(fout_v.at[h], fin_v.at[core, h], fin_send.at[h], fin_recv.at[h], mate)

    def rs_end(h):
        slot = lax.rem(h, 2)
        pre_copy(h, 0).wait_recv()
        for ch in (0, 1):
            for d in (UP, DOWN):
                rs_copy(h, d, ch, chain_len(ch) - 1).wait_recv()
        factor = jnp.where(core == 0, scale, 1.0).astype(F32)
        for half in (0, 1):
            up = ring_v[h, UP, rs_index(half, chain_len(half) - 1)]
            dn = ring_v[h, DOWN, rs_index(1 - half, chain_len(1 - half) - 1)]
            total = (part_v[slot, core, 0, half] + pre_v[h, 0, half] + up + dn) * factor
            done = total.astype(BF)

            @pl.when(core == half)
            def _():
                fin_v[core, h] = done

            @pl.when(core != half)
            def _():
                fout_v[h] = done
        fin_copy(h).start()
        remote(ring_v.at[h], ring_v.at[h], rs_send.at[h], rs_recv.at[h, 0, 0], near[UP]).wait_send()
        remote(pre_v.at[h], pre_v.at[h], pre_send.at[h], pre_recv.at[h, 0], mate).wait_send()

    def project_q(h, slot):
        q_v[h] = mm(x_v[...], wq_v[slot]).astype(BF)

    do_cut = (gcol // 2 + chunk - 1) // chunk * chunk

    def project_do(h, slot, part=None):
        cols = {None: slice(0, gcol), 0: slice(0, do_cut), 1: slice(do_cut, gcol)}[part]
        do_v[h, :, cols] = mm_nt(dy_v[...], wo_v[slot, cols, :]).astype(BF)

    def transpose_kv(h):
        for e in range(n_dev):
            c, cols = e // 2, slice((e % 2) * tok, (e % 2 + 1) * tok)
            kt_v[c, :, cols] = kv_v[h, e, 0].T
            vt_v[c, :, cols] = kv_v[h, e, 1].T

    blk = 16
    n_blk = tok // blk

    def attend(h, serve):
        row_max, delta = {}, {}

        def lanes(j):
            return slice(j * hd, (j + 1) * hd)

        def rows(j):
            return slice(j * tok, (j + 1) * tok)

        def scores(j, i, state):
            if i == 0:
                qt_v[:, lanes(j)] = q_v[h, :, lanes(j)].T
                dot_v[:, lanes(j)] = do_v[h, :, lanes(j)].T
            s = mm(q_v[h, :, lanes(j)], kt_v[i]) * scale2
            s_v[j % 2, i] = s
            top = jnp.maximum(s[:, :hd], s[:, hd:])
            state["top"] = top if i == 0 else jnp.maximum(state["top"], top)
            if i == n_chip - 1:
                row_max[j] = jnp.max(state["top"], axis=1, keepdims=True)

        def exps(j, i, state):
            r = slice(i * blk, (i + 1) * blk)
            total = None
            for c in range(n_chip):
                e = jnp.exp2(s_v[j % 2, c, r, :] - row_max[j][r])
                s_v[j % 2, c, r, :] = e
                both = e[:, :hd] + e[:, hd:]
                total = both if total is None else total + both
            state[i] = 1.0 / jnp.sum(total, axis=1, keepdims=True)

        def probs(j, i, state):
            r = slice(i * blk, (i + 1) * blk)
            for c in range(n_chip):
                p_v[c, j * tok + i * blk:j * tok + (i + 1) * blk, :] = (s_v[j % 2, c, r, :] * state[i]).astype(BF)

        def kv_chunk(i, which):
            return kv_v[h, 2 * i:2 * i + 2, which].reshape(chunk, hd)

        def add_to(state, name, term):
            state[name] = term if name not in state else state[name] + term

        for b in range(-2, q_group + 1):
            state = {}
            soft = {}
            serve(b)
            for i in range(n_chip + 1):
                if i < n_chip and 0 <= b - 1 < q_group:
                    add_to(state, "dq", mm(ds_v[i, rows(b - 1), :], kv_chunk(i, 0)))
                if i < n_chip and 0 <= b + 2 < q_group:
                    scores(b + 2, i, state)
                if 0 <= b + 1 < q_group:
                    if i < n_blk:
                        exps(b + 1, i, soft)
                    if i > 0:
                        probs(b + 1, i - 1, soft)
            if 0 <= b - 1 < q_group:
                do_v[h, :, lanes(b - 1)] = (state["dq"] * scale).astype(BF)
            for i in range(n_chip):
                if 0 <= b + 1 < q_group:
                    add_to(state, "out", mm(p_v[i, rows(b + 1), :], kv_chunk(i, 1)))
                if 0 <= b < q_group:
                    dp = mm(do_v[h, :, lanes(b)], vt_v[i])
                    ds_v[i, rows(b), :] = (p_v[i, rows(b), :].astype(F32) * (dp - delta[b])).astype(BF)
            if 0 <= b + 1 < q_group:
                out = state["out"].astype(BF)
                q_v[h, :, lanes(b + 1)] = out
                do_j = do_v[h, :, lanes(b + 1)].astype(F32)
                delta[b + 1] = jnp.sum(out.astype(F32) * do_j, axis=1, keepdims=True)

    def key_grads(h):
        slot = lax.rem(h, 2)
        order = [far]
        for dist in range(far - 1, 0, -1):
            order += [dist, -dist]
        order.append(0)
        for group in (order[:3], order[3:]):
            for off in group:
                c = chip_at(off)
                gk = mm(qt_v[...], ds_v[c])
                gv = mm(dot_v[...], p_v[c])
                for half in (0, 1):
                    part_v[slot, 0, slot_of(off), half] = gk[:, half * tok:(half + 1) * tok]
                    part_v[slot, 1, slot_of(off), half] = gv[:, half * tok:(half + 1) * tok]
            for off in group:
                pre_copy(h, off).start()

    def outputs_y(h, slot):
        for b in range(n_piece):
            cols = slice(b * gcol, (b + 1) * gcol)
            yacc_v[:, cols] += mm(q_v[h], wo_v[slot, :, cols])

    def outputs_dx(h, slot):
        for b in range(n_piece):
            cols = slice(b * gcol, (b + 1) * gcol)
            dxacc_v[:, cols] += mm_nt(do_v[h], wq_v[slot, cols, :])

    x_copy = pltpu.make_async_copy(x_hbm, x_v, in_sem.at[0])
    dy_copy = pltpu.make_async_copy(dy_hbm, dy_v, in_sem.at[1])
    x_copy.start()
    wk_in = small_copies(wk_hbm, p_v, 0)
    wv_in = small_copies(wv_hbm, ds_v, n_chip)
    for copy in wk_in:
        copy.start()

    barrier = pltpu.get_barrier_semaphore()
    for dev in near + next_near + (mate,):
        pl.semaphore_signal(barrier, inc=1, device_id={"cp": dev}, device_id_type=MESH)

    yacc_v[...] = jnp.zeros_like(yacc_v)
    dxacc_v[...] = jnp.zeros_like(dxacc_v)
    for copy in wv_in:
        copy.start()
    x_copy.wait()

    def project_small(buf, which):
        acc = [None, None]
        for i in range(n_chip):
            b, half = i // 2, i % 2
            term = mm(x_v[:, b * gcol:(b + 1) * gcol], buf[i])
            acc[half] = term if b == 0 else acc[half] + term
        for h in range(kv_heads):
            col = (h % 2) * hd
            kv_v[h, me, which] = acc[h // 2][:, col:col + hd].astype(BF)

    for copy in wk_in:
        copy.wait()
    slab_q(2, 0).start()
    project_small(p_v, 0)
    for copy in wv_in:
        copy.wait()
    dy_copy.start()
    project_small(ds_v, 1)
    slab_o(2, 0).start()
    pl.semaphore_wait(barrier, 5)
    ag_start(0, True)

    slab_q(2, 0).wait()
    slab_q(1, 1).start()
    project_q(2, 0)
    slab_o(1, 1).start()
    dy_copy.wait()
    slab_o(2, 0).wait()
    slab_q(0, 0).start()
    project_do(2, 0)
    slab_o(0, 0).start()
    slab_q(1, 1).wait()
    project_q(1, 1)
    ag_level(0, 2, True)
    ag_level(0, 1, True)
    ag_start(1, True)
    slab_o(1, 1).wait()
    project_do(1, 1)
    slab_q(0, 0).wait()
    project_q(0, 0)
    ag_level(0, 3, True)
    slab_o(0, 0).wait()
    project_do(0, 0)
    ag_level(0, 4, True)

    first_serve = {-2: [(1, 2)], 1: [(1, 1)], 4: [(1, 3)], 6: [(1, 4)], 7: [(2, 1)]}

    def head_step(h, carry):
        def serve(b):
            if b in first_serve:
                @pl.when(h == 0)
                def _():
                    for g, hop in first_serve[b]:
                        ag_level(g, hop, g < 2)
                    if b in (1, 4):
                        ag_start(2 if b == 1 else 3)
            if b in (-1, 2, 4, 5, 7):
                @pl.when(h == 1)
                def _():
                    if b == -1:
                        rs_step(h - 1, 0, 1)
                    elif b == 2:
                        rs_step(h - 1, 1, 1)
                    elif b == 4:
                        ag_level(2, 3)
                    elif b == 5:
                        rs_step(h - 1, 0, 2)
                    else:
                        rs_step(h - 1, 1, 2)
                        ag_level(3, 2)
            if b in (1, 5, 6, 7):
                @pl.when(h == 2)
                def _():
                    if b == 1:
                        ag_level(3, 3)
                    elif b == 5:
                        rs_step(h - 1, 0, 1)
                    elif b == 6:
                        rs_step(h - 1, 1, 1)
                    else:
                        rs_end(h - 2)
                        ag_level(3, 4)
            if b in (1, 3, 7):
                @pl.when(h == 3)
                def _():
                    if b == 1:
                        rs_step(h - 2, 0, 3)
                        rs_step(h - 1, 0, 1)
                    elif b == 3:
                        rs_step(h - 1, 1, 1)
                    else:
                        rs_step(h - 1, 0, 2)
                        rs_end(h - 2)

        ag_finish(h)
        transpose_kv(h)
        attend(h, serve)
        key_grads(h)

        @pl.when(h == 1)
        def _():
            ag_level(2, 4)
            rs_step(h - 1, 0, 3)

        @pl.when(h == 2)
        def _():
            rs_step(h - 1, 0, 2)

        rs_begin(h)

        @pl.when(h == 0)
        def _():
            ag_level(3, 1)
            outputs_y(h, 0)
            slab_o(3, 0).start()
            ag_level(2, 2)
            outputs_dx(h, 0)
            slab_q(3, 0).start()

        @pl.when(h == 2)
        def _():
            slab_q(3, 0).wait()
            project_q(3, 0)
            rs_step(h - 1, 1, 2)
            slab_o(3, 0).wait()
            project_do(3, 0)

        return carry

    lax.fori_loop(0, kv_heads, head_step, 0)

    last = kv_heads - 1
    wk_in = small_copies(wk_hbm, p_v, 0)
    wv_in = small_copies(wv_hbm, ds_v, n_chip)
    for copy in wk_in + wv_in:
        copy.start()

    def fin_wait(h):
        remote(fout_v.at[h], fin_v.at[1 - core, h], fin_send.at[h], fin_recv.at[h], mate).wait_recv()

    def dx_copy(b):
        cols = pl.ds(b * gcol, gcol)
        return pltpu.make_async_copy(dy_v.at[:, cols], dx_hbm.at[:, cols], out_sem.at[b])

    def key_outputs(half, store):
        pair = (2 * half, 2 * half + 1)
        gk = jnp.concatenate([fin_v[0, h].T for h in pair], axis=1)
        gv = jnp.concatenate([fin_v[1, h].T for h in pair], axis=1)
        for b in range(n_piece):
            cols = slice(b * gcol, (b + 1) * gcol)
            i = 2 * b + half
            total = dxacc_v[:, cols] + mm_nt(gk, p_v[i]) + mm_nt(gv, ds_v[i])
            if store:
                dy_v[:, cols] = total.astype(BF)
                dx_copy(b).start()
            else:
                dxacc_v[:, cols] = total

    rs_step(2, 1, 2)
    outputs_y(1, 1)
    rs_step(2, 0, 3)
    slab_o(2, 1).start()
    outputs_dx(1, 1)
    slab_q(2, 1).start()
    rs_step(3, 0, 1)
    outputs_y(3, 0)
    rs_step(3, 1, 1)
    outputs_dx(3, 0)
    rs_end(2)
    rs_step(3, 0, 2)
    slab_o(2, 1).wait()
    outputs_y(2, 1)
    x_v[...] = yacc_v[...].astype(BF)
    y_copy = pltpu.make_async_copy(x_v, y_hbm, in_sem.at[0])
    y_copy.start()
    rs_step(3, 1, 2)
    for copy in wk_in + wv_in:
        copy.wait()
    fin_wait(0)
    fin_wait(1)
    key_outputs(0, False)
    rs_step(3, 0, 3)
    slab_q(2, 1).wait()
    outputs_dx(2, 1)
    for h in range(kv_heads):
        ag_drain(h)
    rs_end(3)
    fin_wait(2)
    fin_wait(3)
    key_outputs(1, True)
    for h in range(kv_heads):
        fin_copy(h).wait_send()
    y_copy.wait()
    for b in range(n_piece):
        dx_copy(b).wait()


def store_kernel(y_in, dx_in, y_out, dx_out, buf, in_sem, out_sem):
    n_part, rows = buf.shape[0] // 2, buf.shape[1]
    pairs = []
    for i in range(2 * n_part):
        src, dst = ((y_in, y_out), (dx_in, dx_out))[i // n_part]
        at = pl.ds((i % n_part) * rows, rows)
        pairs.append((pltpu.make_async_copy(src.at[at], buf.at[i], in_sem.at[i]),
                      pltpu.make_async_copy(buf.at[i], dst.at[at], out_sem.at[i])))
    for take, _ in pairs:
        take.start()
    for take, give in pairs:
        take.wait()
        give.start()
    for _, give in pairs:
        give.wait()


def solution(mesh):
    n_dev = mesh.shape["cp"]
    row_spec = P(("dp", "cp"), None)
    full_spec = P(None, None)

    def local_body(x_loc, dy_loc, w_q, w_k, w_v, w_o):
        tok, width = x_loc.shape
        q_heads = w_q.shape[1] // HEAD_DIM
        kv_heads = w_k.shape[1] // HEAD_DIM
        q_group = q_heads // kv_heads
        gcol = q_group * HEAD_DIM
        n_chip = n_dev // 2
        far = n_chip // 2
        chunk = 2 * tok
        hd = HEAD_DIM
        any_spec = pl.BlockSpec(memory_space=pl.ANY)
        dma = pltpu.SemaphoreType.DMA
        scratch = [
            pltpu.VMEM((tok, width), BF), pltpu.VMEM((tok, width), BF),
            pltpu.VMEM((2, width, gcol), BF), pltpu.VMEM((2, gcol, width), BF),
            pltpu.VMEM((kv_heads, n_dev, 2, tok, hd), BF),
            pltpu.VMEM((n_chip, hd, chunk), BF), pltpu.VMEM((n_chip, hd, chunk), BF),
            pltpu.VMEM((kv_heads, tok, gcol), BF), pltpu.VMEM((kv_heads, tok, gcol), BF),
            pltpu.VMEM((hd, q_group * tok), BF), pltpu.VMEM((hd, q_group * tok), BF),
            pltpu.VMEM((2, n_chip, tok, chunk), F32),
            pltpu.VMEM((n_chip, q_group * tok, chunk), BF), pltpu.VMEM((n_chip, q_group * tok, chunk), BF),
            pltpu.VMEM((2, 2, n_chip, 2, hd, tok), F32), pltpu.VMEM((kv_heads, n_chip, 2, hd, tok), F32),
            pltpu.VMEM((kv_heads, 2, 2 * far - 1, hd, tok), F32),
            pltpu.VMEM((tok, width), F32), pltpu.VMEM((tok, width), F32),
            pltpu.VMEM((2, kv_heads, hd, tok), BF), pltpu.VMEM((kv_heads, hd, tok), BF),
            dma((2,)), dma((2 * n_chip,)), dma((2, 2)),
            dma((kv_heads,)), dma((kv_heads, 4 * far + 1)),
            dma((kv_heads,)), dma((kv_heads, n_chip)),
            dma((kv_heads,)), dma((kv_heads, 2, 2 * far - 1)),
            dma((kv_heads,)), dma((kv_heads,)), dma((width // gcol,)),
        ]
        out = jax.ShapeDtypeStruct((tok, width), BF)
        y, dx = pl.pallas_call(
            functools.partial(layer_kernel, n_dev, kv_heads, q_group),
            out_shape=(out, out),
            in_specs=[any_spec] * 6,
            out_specs=(any_spec, any_spec),
            scratch_shapes=scratch,
            name="layer",
            compiler_params=pltpu.CompilerParams(collective_id=0, has_side_effects=True,
                                                 vmem_limit_bytes=67043328),
        )(x_loc, dy_loc, w_q, w_k, w_v, w_o)
        n_part = 2
        return pl.pallas_call(
            store_kernel,
            out_shape=(out, out),
            in_specs=[any_spec] * 2,
            out_specs=(any_spec, any_spec),
            scratch_shapes=[pltpu.VMEM((2 * n_part, tok // n_part, width), BF),
                            dma((2 * n_part,)), dma((2 * n_part,))],
            name="store",
        )(y, dx)

    return jax.shard_map(local_body, mesh=mesh,
                         in_specs=(row_spec, row_spec, full_spec, full_spec, full_spec, full_spec),
                         out_specs=(row_spec, row_spec), check_vma=False)
```
